256 devices in a mesh: row: 8 (over x, core), col: 32 (over y, z).
Axes of the slice: x: 4, y: 4, z: 8, core: 2. Of those that a mesh axis runs over, the one named last changes fastest.
Arguments:
- matrix: float32 [2048, 65536], P('col', 'row'), may hold values from -6 to 6
- basis: float32 [65536, 512], P(('row', 'col')), may hold values from -0.0234375 to 0.0234375
Outputs:
- root: float32 [512, 512], P('row', 'col')
- right: float32 [2048, 512], P('col')
The draws below stay inside these ranges and needn't reach their ends.
All inputs are finite; a program needn't handle non-finite values.
Results may differ from the reference program's by a relative error of at most 0.00018.
Values sent between devices are 32-bit elements; how exact they have to be, the bound alone decides.
A program may use at most 64 MiB of HBM per device.

```python
import jax
import jax.numpy as jnp
from jax import lax

N = 2048
K = 512
ITERS = 8
M = 65536


def steps_of(own_key, extent, split, smallest, largest):
    def one(axis_at, shards_of):
        draws = jax.random.uniform(jax.random.fold_in(jax.random.fold_in(own_key, 6), axis_at), (shards_of,), jnp.float32, smallest / len(split), largest / len(split))
        return jnp.repeat(jnp.exp(draws), extent[axis_at] // shards_of).reshape((-1,) + (1,) * (len(extent) - axis_at - 1))

    gain = one(*split[0])
    for cut in split[1:]:
        gain = gain * one(*cut)
    return gain


def noise(stream_key, dims, width, bound, cuts=(), kind=jnp.bfloat16):
    level = steps_of(stream_key, dims, cuts, -0.22, 0.18) if cuts else 1.0
    drawn = jax.random.normal(stream_key, dims, jnp.float32) * width * level
    return jnp.minimum(jnp.maximum(drawn, -bound), bound).astype(kind)


def setup_inputs(seed: int = 0) -> dict:
    seeds = jax.random.split(jax.random.key(seed), 3)
    matrix = noise(seeds[0], (N, M), 1.0, 6.0, ((0, 32), (1, 8)), jnp.float32)
    basis = noise(seeds[1], (M, K), M ** -0.5, 0.0234375, ((0, 256),), jnp.float32)
    return dict(matrix=matrix, basis=basis)


def reference(matrix, basis):
    highest = lax.Precision.HIGHEST
    proj = lax.dot_general(basis, matrix, (((0,), (1,)), ((), ())), precision=highest)
    gram = jnp.dot(proj, proj.T, precision=highest)
    scale = jnp.sqrt(jnp.sum(gram * gram) + 1e-06)
    ident = jnp.eye(K, dtype=jnp.float32)
    upper = gram / scale
    lower = ident
    for step in range(ITERS):
        middle = 0.5 * (3.0 * ident - jnp.dot(lower, upper, precision=highest))
        upper = jnp.dot(upper, middle, precision=highest)
        lower = jnp.dot(middle, lower, precision=highest)
    root_scale = jnp.sqrt(scale)
    root = upper * root_scale
    right = jnp.dot(proj.T, lower, precision=highest) / root_scale
    return (root, right)
```

```python
import functools

import jax
import jax.numpy as jnp
from jax import lax
from jax.experimental import pallas as pl
from jax.experimental.pallas import tpu as pltpu
from jax.sharding import PartitionSpec as P

MESH = pl.DeviceIdType.MESH
ITERS = 8
F32 = jnp.float32
BF16 = jnp.bfloat16
NX, NY, NZ = 4, 4, 8
NR, PLANE = 2 * NX, 2 * NX * NY


def split(a):
    hi = a.astype(BF16)
    return hi, (a - hi.astype(F32)).astype(BF16)


def product(ah, al, bh, bl, dims=(((1,), (0,)), ((), ()))):
    dot = functools.partial(
        lax.dot_general, dimension_numbers=dims, preferred_element_type=F32
    )
    return dot(ah, bh) + (dot(ah, bl) + dot(al, bh))


def lanes(i, size):
    return pl.ds(pl.multiple_of(i * size, size), size)


def gather_kernel(
    mat, bas, gram, own_cols,
    m_in, m_hi, m_lo, q, acc, land, proj, block, zland,
    y_send, y_recv, f_send, f_recv, b_send, b_recv, local_sem,
    p_send, p_recv, a_send, a_recv, z_send, z_recv, g_send, g_recv, d_send, d_recv,
):
    r, c = lax.axis_index("row"), lax.axis_index("col")
    y, z = c // NZ, c % NZ
    x, core = r // 2, r % 2
    cols = mat.shape[0]
    part = mat.shape[1] // NY
    rows, width = bas.shape
    half = rows // 2
    wide = width // 4
    piece = cols // NR

    def plane_peer(k):
        return (r + k // NY) % NR, (y + k % NY) % NY

    def z_peer(k):
        return (r, y * NZ + (z + k) % NZ)

    barrier = pltpu.get_barrier_semaphore()

    def greet_plane(k, _):
        r2, y2 = plane_peer(k)
        pl.semaphore_signal(barrier, inc=1, device_id=(r2, y2 * NZ + z), device_id_type=MESH)
        return 0

    def greet_z(k, _):
        pl.semaphore_signal(barrier, inc=1, device_id=z_peer(k), device_id_type=MESH)
        return 0

    lax.fori_loop(1, PLANE, greet_plane, 0)
    lax.fori_loop(1, NZ, greet_z, 0)
    pl.semaphore_wait(barrier, PLANE - 1 + NZ - 1)

    def ring_copy(m, d, ahead):
        sign = 1 if ahead else -1
        owner = (z - sign * d + NZ) % NZ
        here = pl.ds(m * wide, wide)
        if d == 0:
            src = bas.at[:, here]
            dst = q.at[lanes(owner, rows), here]
        else:
            span = pl.ds(pl.multiple_of(owner * rows, rows), rows)
            if d == 3:
                start = owner * rows + (0 if ahead else half)
                span = pl.ds(pl.multiple_of(start, half), half)
            src = dst = q.at[span, here]
        send, recv = (f_send, f_recv) if ahead else (b_send, b_recv)
        return pltpu.make_async_remote_copy(
            src_ref=src, dst_ref=dst, send_sem=send.at[m, d], recv_sem=recv.at[m, d],
            device_id=(r, y * NZ + (z + sign + NZ) % NZ), device_id_type=MESH,
        )

    def ring_wait(m, d, ahead):
        sign = 1 if ahead else -1
        owner = (z - sign * (d + 1) + NZ) % NZ
        here = pl.ds(m * wide, wide)
        span = pl.ds(pl.multiple_of(owner * rows, rows), rows)
        if d == 3:
            start = owner * rows + (0 if ahead else half)
            span = pl.ds(pl.multiple_of(start, half), half)
        send, recv = (f_send, f_recv) if ahead else (b_send, b_recv)
        pltpu.make_async_remote_copy(
            src_ref=q.at[span, here], dst_ref=q.at[span, here],
            send_sem=send.at[m, d], recv_sem=recv.at[m, d],
            device_id=(r, y * NZ + (z + sign + NZ) % NZ), device_id_type=MESH,
        ).wait_recv()

    def y_copy(k):
        y2 = (y + k) % NY
        return pltpu.make_async_remote_copy(
            src_ref=mat.at[:, lanes(y2, part)], dst_ref=m_in.at[lanes(y, cols), :],
            send_sem=y_send.at[k - 1], recv_sem=y_recv.at[k - 1],
            device_id=(r, y2 * NZ + z), device_id_type=MESH,
        )

    def y_wait(k):
        src = (y - k + NY) % NY
        pltpu.make_async_remote_copy(
            src_ref=mat.at[:, lanes(src, part)], dst_ref=m_in.at[lanes(src, cols), :],
            send_sem=y_send.at[k - 1], recv_sem=y_recv.at[k - 1],
            device_id=(r, src * NZ + z), device_id_type=MESH,
        ).wait_recv()

    copies = []

    def issue(m, d):
        for ahead in (True, False):
            if d > 0:
                ring_wait(m, d - 1, ahead)
            copy = ring_copy(m, d, ahead)
            copy.start()
            copies.append(copy)

    def split_rows(src):
        def one(i, _):
            at = pl.ds(pl.multiple_of(i * 16, 16), 16)
            hi, lo = split(m_in[at, :])
            m_hi[at, :] = hi
            m_lo[at, :] = lo
            return 0

        lax.fori_loop(src * (cols // 16), (src + 1) * (cols // 16), one, 0)

    def own_split(i, _):
        hi, lo = split(mat[pl.ds(pl.multiple_of(i * 16, 16), 16), lanes(y, part)])
        at = pl.ds(pl.multiple_of(y * cols + i * 16, 16), 16)
        m_hi[at, :] = hi
        m_lo[at, :] = lo
        return 0

    def multiply(pair, first, last):
        here = pl.ds(pair * 2 * wide, 2 * wide)

        def one(o, _):
            owner = (z + o) % NZ
            qh, ql = split(q[lanes(owner, rows), here])
            at = lanes(owner, rows)
            acc[:, here] += product(m_hi[:, at], m_lo[:, at], qh, ql)
            return 0

        lax.fori_loop(first, last, one, 0)

    def spread_partial(pair):
        here = pl.ds(pair * 2 * wide, 2 * wide)

        def one(k, _):
            r2, y2 = plane_peer(k)
            src = pl.ds(pl.multiple_of(y2 * cols + r2 * piece, piece), piece)
            pltpu.make_async_remote_copy(
                src_ref=acc.at[src, here], dst_ref=land.at[lanes(k - 1, piece), here],
                send_sem=p_send.at[pair], recv_sem=p_recv.at[pair],
                device_id=(r2, y2 * NZ + z), device_id_type=MESH,
            ).start()
            return 0

        lax.fori_loop(1, PLANE, one, 0)

    mine = pl.ds(pl.multiple_of(y * cols + r * piece, piece), piece)

    def all_of(ref, pair, send, recv):
        here = pl.ds(pair * 2 * wide, 2 * wide)
        view = ref.at[pl.ds(0, (PLANE - 1) * piece), here]
        return pltpu.make_async_remote_copy(
            src_ref=view, dst_ref=view, send_sem=send.at[pair], recv_sem=recv.at[pair],
            device_id=z_peer(1), device_id_type=MESH,
        )

    def total_and_spread(pair):
        here = pl.ds(pair * 2 * wide, 2 * wide)
        all_of(land, pair, p_send, p_recv).wait_recv()
        total = acc[mine, here]
        for k in range(PLANE - 1):
            total = total + land[pl.ds(k * piece, piece), here]
        proj[mine, here] = total

        def one(k, _):
            r2, y2 = plane_peer(k)
            pltpu.make_async_remote_copy(
                src_ref=proj.at[mine, here], dst_ref=proj.at[mine, here],
                send_sem=a_send.at[pair], recv_sem=a_recv.at[pair],
                device_id=(r2, y2 * NZ + z), device_id_type=MESH,
            ).start()
            return 0

        lax.fori_loop(1, PLANE, one, 0)

    own = pltpu.make_async_copy(bas, q.at[lanes(z, rows), :], local_sem)
    own.start()
    issue(0, 0)
    for k in range(1, NY):
        y_copy(k).start()
    issue(1, 0)
    acc[...] = jnp.zeros_like(acc)
    lax.fori_loop(0, cols // 16, own_split, 0)
    own.wait()
    for d in range(1, 4):
        issue(0, d)
        issue(1, d)
    issue(2, 0)
    issue(3, 0)
    issue(2, 1)
    issue(3, 1)
    issue(2, 2)
    for k in range(1, NY):
        y_wait(k)
        split_rows((y - k + NY) % NY)
    for m in (0, 1):
        for ahead in (True, False):
            ring_wait(m, 3, ahead)
    multiply(0, 0, NZ)
    spread_partial(0)
    issue(3, 2)
    multiply(1, 0, 3)
    issue(2, 3)
    issue(3, 3)
    multiply(1, 3, 4)
    multiply(1, 5, NZ)
    total_and_spread(0)
    for m in (2, 3):
        for ahead in (True, False):
            ring_wait(m, 3, ahead)
    multiply(1, 4, 5)
    spread_partial(1)
    total_and_spread(1)
    for pair in (0, 1):
        all_of(proj, pair, a_send, a_recv).wait_recv()
    own_cols[...] = proj[lanes(y, cols), :]

    side = width // 4
    lh, ll = split(proj[:, lanes(y, side)].T)
    rh, rl = split(proj[:, lanes(x, side)])
    block[...] = product(lh, ll, rh, rl)
    low = side // 2
    my_half = pl.ds(pl.multiple_of(core * low, low), low)
    zland[lanes(z, low), :] = block[my_half, :]

    def to_z(k, _):
        pltpu.make_async_remote_copy(
            src_ref=block.at[my_half, :], dst_ref=zland.at[lanes(z, low), :],
            send_sem=z_send, recv_sem=z_recv, device_id=z_peer(k), device_id_type=MESH,
        ).start()
        return 0

    lax.fori_loop(1, NZ, to_z, 0)
    view = zland.at[pl.ds(0, (NZ - 1) * low), :]
    z_all = pltpu.make_async_remote_copy(
        src_ref=view, dst_ref=view, send_sem=z_send, recv_sem=z_recv,
        device_id=z_peer(1), device_id_type=MESH,
    )
    z_all.wait_recv()
    total = zland[pl.ds(0, low), :]
    for k in range(1, NZ):
        total = total + zland[pl.ds(k * low, low), :]

    def gram_rows(y2):
        return pl.ds(pl.multiple_of(y2 * side + core * low, low), low)

    here = lanes(x, side)
    gram[gram_rows(y), here] = total
    for k in range(1, NX * NY):
        kx, ky = k % NX, k // NX
        r2 = ((x + kx) % NX) * 2 + core
        pltpu.make_async_remote_copy(
            src_ref=gram.at[gram_rows(y), here], dst_ref=gram.at[gram_rows(y), here],
            send_sem=g_send, recv_sem=g_recv.at[ky],
            device_id=(r2, ((y + ky) % NY) * NZ + z), device_id_type=MESH,
        ).start()
    partner = (x * 2 + 1 - core, c)
    crossings = []
    for ky in range(NY):
        y2 = (y - ky + NY) % NY
        count = (NX - 1 if ky == 0 else NX) * side
        view = gram.at[gram_rows(y2), pl.ds(0, count)]
        pltpu.make_async_remote_copy(
            src_ref=view, dst_ref=view, send_sem=g_send, recv_sem=g_recv.at[ky],
            device_id=partner, device_id_type=MESH,
        ).wait_recv()
        copy = pltpu.make_async_remote_copy(
            src_ref=gram.at[gram_rows(y2), :], dst_ref=gram.at[gram_rows(y2), :],
            send_sem=d_send.at[ky], recv_sem=d_recv.at[ky],
            device_id=partner, device_id_type=MESH,
        )
        copy.start()
        crossings.append(copy)
    for ky in range(NY):
        y2 = (y - ky + NY) % NY
        theirs = pl.ds(pl.multiple_of(y2 * side + (1 - core) * low, low), low)
        pltpu.make_async_remote_copy(
            src_ref=gram.at[theirs, :], dst_ref=gram.at[theirs, :],
            send_sem=d_send.at[ky], recv_sem=d_recv.at[ky],
            device_id=partner, device_id_type=MESH,
        ).wait_recv()

    for copy in copies + crossings:
        copy.wait_send()
    for k in range(1, NY):
        y_copy(k).wait_send()
    for pair in (0, 1):
        all_of(land, pair, p_send, p_recv).wait_send()
        all_of(proj, pair, a_send, a_recv).wait_send()
    z_all.wait_send()
    view = zland.at[pl.ds(0, low), :]
    for k in range(1, NX * NY):
        pltpu.make_async_remote_copy(
            src_ref=view, dst_ref=view, send_sem=g_send, recv_sem=g_recv.at[0],
            device_id=partner, device_id_type=MESH,
        ).wait_send()


def gather(matrix, basis):
    cols, depth = matrix.shape
    rows, width = basis.shape
    part = depth // NY
    side = width // 4
    dma = pltpu.SemaphoreType.DMA
    vmem = pl.BlockSpec(memory_space=pltpu.VMEM)
    return pl.pallas_call(
        gather_kernel,
        name="gather",
        out_shape=(
            jax.ShapeDtypeStruct((width, width), F32),
            jax.ShapeDtypeStruct((cols, width), F32),
        ),
        in_specs=[vmem, vmem],
        out_specs=(vmem, vmem),
        scratch_shapes=[
            pltpu.VMEM((NY * cols, part), F32),
            pltpu.VMEM((NY * cols, part), BF16),
            pltpu.VMEM((NY * cols, part), BF16),
            pltpu.VMEM((NZ * rows, width), F32),
            pltpu.VMEM((NY * cols, width), F32),
            pltpu.VMEM(((PLANE - 1) * cols // NR, width), F32),
            pltpu.VMEM((NY * cols, width), F32),
            pltpu.VMEM((side, side), F32),
            pltpu.VMEM((NZ * side // 2, side), F32),
            dma((NY - 1,)), dma((NY - 1,)),
            dma((4, 4)), dma((4, 4)), dma((4, 4)), dma((4, 4)), dma,
            dma((2,)), dma((2,)), dma((2,)), dma((2,)),
            dma, dma, dma, dma((NY,)), dma((NY,)), dma((NY,)),
        ],
        compiler_params=pltpu.CompilerParams(
            collective_id=0, has_side_effects=True, vmem_limit_bytes=48 * 2**20
        ),
    )(matrix, basis)


def polar_kernel(gram, own_cols, root, right, t, t_hi, t_lo, b_hi, b_lo, v):
    r, c = lax.axis_index("row"), lax.axis_index("col")
    width = gram.shape[0]
    cols = own_cols.shape[0]
    row_len = root.shape[0]
    total = jnp.sum(gram[...] * gram[...])
    scale = jnp.sqrt(jnp.full((1, 1), total, F32) + 1e-06)
    root_scale = jnp.sqrt(scale)
    t[...] = gram[...] / scale
    v[pl.ds(0, cols), :] = own_cols[...]
    v[pl.ds(cols, row_len), :] = gram[lanes(r, row_len), :] / scale

    def split_t():
        hi, lo = split(t[...])
        t_hi[...] = hi
        t_lo[...] = lo

    def advance():
        vh, vl = split(v[...])
        v[...] = 1.5 * v[...] - 0.5 * product(vh, vl, t_hi[...], t_lo[...])

    def step(_, carry):
        split_t()
        advance()
        b = product(t_hi[...], t_lo[...], t_hi[...], t_lo[...])
        hi, lo = split(b)
        b_hi[...] = hi
        b_lo[...] = lo
        t[...] = (2.25 * t[...] - 1.5 * b) + 0.25 * product(
            b_hi[...], b_lo[...], t_hi[...], t_lo[...]
        )
        return carry

    lax.fori_loop(0, ITERS - 1, step, 0)
    split_t()
    advance()
    right[...] = v[pl.ds(0, cols), :] / root_scale
    ours = v[pl.ds(cols, row_len), :] * root_scale
    col_len = root.shape[1]
    turn = (width - c * col_len) % width
    root[...] = pltpu.roll(ours, turn, 1)[:, :col_len]


def polar(gram, own_cols, row_len, col_len):
    width = gram.shape[0]
    cols = own_cols.shape[0]
    vmem = pl.BlockSpec(memory_space=pltpu.VMEM)
    return pl.pallas_call(
        polar_kernel,
        name="polar",
        out_shape=(
            jax.ShapeDtypeStruct((row_len, col_len), F32),
            jax.ShapeDtypeStruct((cols, width), F32),
        ),
        in_specs=[vmem, vmem],
        out_specs=(vmem, vmem),
        scratch_shapes=[
            pltpu.VMEM((width, width), F32),
            pltpu.VMEM((width, width), BF16),
            pltpu.VMEM((width, width), BF16),
            pltpu.VMEM((width, width), BF16),
            pltpu.VMEM((width, width), BF16),
            pltpu.VMEM((cols + row_len, width), F32),
        ],
    )(gram, own_cols)


def local(matrix, basis):
    width = basis.shape[1]
    gram, own_cols = gather(matrix, basis)
    return polar(
        gram, own_cols, width // lax.axis_size("row"), width // lax.axis_size("col")
    )


def solution(mesh):
    return jax.shard_map(
        local,
        mesh=mesh,
        in_specs=(P("col", "row"), P(("row", "col"), None)),
        out_specs=(P("row", "col"), P("col", None)),
        check_vma=False,
    )
```

```python
import functools

import jax
import jax.numpy as jnp
from jax import lax
from jax.experimental import pallas as pl
from jax.experimental.pallas import tpu as pltpu
from jax.sharding import PartitionSpec as P

MESH = pl.DeviceIdType.MESH
ITERS = 8
F32 = jnp.float32
BF16 = jnp.bfloat16
NX, NY, NZ = 4, 4, 8
NR, PLANE = 2 * NX, 2 * NX * NY


def split(a):
    hi = a.astype(BF16)
    return hi, (a - hi.astype(F32)).astype(BF16)


def product(ah, al, bh, bl, dims=(((1,), (0,)), ((), ()))):
    dot = functools.partial(
        lax.dot_general, dimension_numbers=dims, preferred_element_type=F32
    )
    return dot(ah, bh) + (dot(ah, bl) + dot(al, bh))


def lanes(i, size):
    return pl.ds(pl.multiple_of(i * size, size), size)


def step_kernel(
    mat_hbm, bas_hbm, root, right,
    mat, m_in, m_hi, m_lo, q, acc, land, proj, block, own_piece, zland, packed,
    t, t_hi, t_lo, b_hi, b_lo, v,
    y_send, y_recv, f_send, f_recv, b_send, b_recv, local_sem,
    p_send, p_recv, a_send, a_recv, z_send, z_recv, g_send, g_recv, d_send, d_recv,
):
    r, c = lax.axis_index("row"), lax.axis_index("col")
    y, z = c // NZ, c % NZ
    x, core = r // 2, r % 2
    cols = mat.shape[0]
    part = mat.shape[1] // NY
    rows, width = bas_hbm.shape
    half = rows // 2
    wide = width // 4
    piece = cols // NR

    def plane_peer(k):
        return (r + k // NY) % NR, (y + k % NY) % NY

    def z_peer(k):
        return (r, y * NZ + (z + k) % NZ)

    own_basis = pltpu.make_async_copy(bas_hbm, q.at[lanes(z, rows), :], local_sem.at[0])
    own_basis.start()
    own_matrix = pltpu.make_async_copy(mat_hbm, mat, local_sem.at[1])
    own_matrix.start()

    barrier = pltpu.get_barrier_semaphore()

    def greet_plane(k, _):
        r2, y2 = plane_peer(k)
        pl.semaphore_signal(barrier, inc=1, device_id=(r2, y2 * NZ + z), device_id_type=MESH)
        return 0

    def greet_z(k, _):
        pl.semaphore_signal(barrier, inc=1, device_id=z_peer(k), device_id_type=MESH)
        return 0

    lax.fori_loop(1, PLANE, greet_plane, 0)
    lax.fori_loop(1, NZ, greet_z, 0)
    pl.semaphore_wait(barrier, PLANE - 1 + NZ - 1)

    def ring_copy(m, d, ahead):
        sign = 1 if ahead else -1
        owner = (z - sign * d + NZ) % NZ
        here = pl.ds(m * wide, wide)
        span = pl.ds(pl.multiple_of(owner * rows, rows), rows)
        if d == 3:
            start = owner * rows + (0 if ahead else half)
            span = pl.ds(pl.multiple_of(start, half), half)
        send, recv = (f_send, f_recv) if ahead else (b_send, b_recv)
        return pltpu.make_async_remote_copy(
            src_ref=q.at[span, here], dst_ref=q.at[span, here], send_sem=send.at[m, d], recv_sem=recv.at[m, d],
            device_id=(r, y * NZ + (z + sign + NZ) % NZ), device_id_type=MESH,
        )

    def ring_wait(m, d, ahead):
        sign = 1 if ahead else -1
        owner = (z - sign * (d + 1) + NZ) % NZ
        here = pl.ds(m * wide, wide)
        span = pl.ds(pl.multiple_of(owner * rows, rows), rows)
        if d == 3:
            start = owner * rows + (0 if ahead else half)
            span = pl.ds(pl.multiple_of(start, half), half)
        send, recv = (f_send, f_recv) if ahead else (b_send, b_recv)
        pltpu.make_async_remote_copy(
            src_ref=q.at[span, here], dst_ref=q.at[span, here],
            send_sem=send.at[m, d], recv_sem=recv.at[m, d],
            device_id=(r, y * NZ + (z + sign + NZ) % NZ), device_id_type=MESH,
        ).wait_recv()

    def y_copy(k):
        y2 = (y + k) % NY
        return pltpu.make_async_remote_copy(
            src_ref=mat.at[:, lanes(y2, part)], dst_ref=m_in.at[lanes(y, cols), :],
            send_sem=y_send.at[k - 1], recv_sem=y_recv.at[k - 1],
            device_id=(r, y2 * NZ + z), device_id_type=MESH,
        )

    def y_wait(k):
        src = (y - k + NY) % NY
        pltpu.make_async_remote_copy(
            src_ref=mat.at[:, lanes(src, part)], dst_ref=m_in.at[lanes(src, cols), :],
            send_sem=y_send.at[k - 1], recv_sem=y_recv.at[k - 1],
            device_id=(r, src * NZ + z), device_id_type=MESH,
        ).wait_recv()

    copies = []

    def issue(m, d):
        for ahead in (True, False):
            if d > 0:
                ring_wait(m, d - 1, ahead)
            copy = ring_copy(m, d, ahead)
            copy.start()
            copies.append(copy)

    def split_rows(src):
        def one(i, _):
            at = pl.ds(pl.multiple_of(i * 16, 16), 16)
            hi, lo = split(m_in[at, :])
            m_hi[at, :] = hi
            m_lo[at, :] = lo
            return 0

        lax.fori_loop(src * (cols // 16), (src + 1) * (cols // 16), one, 0)

    def own_split(i, _):
        hi, lo = split(mat[pl.ds(pl.multiple_of(i * 16, 16), 16), lanes(y, part)])
        at = pl.ds(pl.multiple_of(y * cols + i * 16, 16), 16)
        m_hi[at, :] = hi
        m_lo[at, :] = lo
        return 0

    def multiply(pair, first, last):
        here = pl.ds(pair * 2 * wide, 2 * wide)

        def one(o, _):
            owner = (z + o) % NZ
            qh, ql = split(q[lanes(owner, rows), here])
            at = lanes(owner, rows)
            acc[:, here] += product(m_hi[:, at], m_lo[:, at], qh, ql)
            return 0

        lax.fori_loop(first, last, one, 0)

    def spread_partial(pair):
        here = pl.ds(pair * 2 * wide, 2 * wide)

        def one(k, _):
            r2, y2 = plane_peer(k)
            src = pl.ds(pl.multiple_of(y2 * cols + r2 * piece, piece), piece)
            pltpu.make_async_remote_copy(
                src_ref=acc.at[src, here], dst_ref=land.at[lanes(k - 1, piece), here],
                send_sem=p_send.at[pair], recv_sem=p_recv.at[pair],
                device_id=(r2, y2 * NZ + z), device_id_type=MESH,
            ).start()
            return 0

        lax.fori_loop(1, PLANE, one, 0)

    mine = pl.ds(pl.multiple_of(y * cols + r * piece, piece), piece)

    def all_of(ref, pair, send, recv):
        here = pl.ds(pair * 2 * wide, 2 * wide)
        view = ref.at[pl.ds(0, (PLANE - 1) * piece), here]
        return pltpu.make_async_remote_copy(
            src_ref=view, dst_ref=view, send_sem=send.at[pair], recv_sem=recv.at[pair],
            device_id=z_peer(1), device_id_type=MESH,
        )

    def total_and_spread(pair):
        here = pl.ds(pair * 2 * wide, 2 * wide)
        all_of(land, pair, p_send, p_recv).wait_recv()
        total = acc[mine, here]
        for k in range(PLANE - 1):
            total = total + land[pl.ds(k * piece, piece), here]
        proj[mine, here] = total

        def one(k, _):
            r2, y2 = plane_peer(k)
            pltpu.make_async_remote_copy(
                src_ref=proj.at[mine, here], dst_ref=proj.at[mine, here],
                send_sem=a_send.at[pair], recv_sem=a_recv.at[pair],
                device_id=(r2, y2 * NZ + z), device_id_type=MESH,
            ).start()
            return 0

        lax.fori_loop(1, PLANE, one, 0)

    own_basis.wait()
    issue(0, 0)
    own_matrix.wait()
    for k in range(1, NY):
        y_copy(k).start()
    issue(1, 0)
    acc[...] = jnp.zeros_like(acc)
    lax.fori_loop(0, cols // 16, own_split, 0)
    for d in range(1, 4):
        issue(0, d)
        issue(1, d)
    issue(2, 0)
    issue(3, 0)
    issue(2, 1)
    issue(3, 1)
    issue(2, 2)
    for k in range(1, NY):
        y_wait(k)
        split_rows((y - k + NY) % NY)
    for m in (0, 1):
        for ahead in (True, False):
            ring_wait(m, 3, ahead)
    multiply(0, 0, NZ)
    spread_partial(0)
    issue(3, 2)
    multiply(1, 0, 3)
    issue(2, 3)
    issue(3, 3)
    multiply(1, 3, 4)
    multiply(1, 5, NZ)
    total_and_spread(0)
    for m in (2, 3):
        for ahead in (True, False):
            ring_wait(m, 3, ahead)
    multiply(1, 4, 5)
    spread_partial(1)
    total_and_spread(1)
    for pair in (0, 1):
        all_of(proj, pair, a_send, a_recv).wait_recv()

    side = width // NY
    low = side // 2
    tile = 8
    s = y * NX + x
    count = 10 * low // tile // (NX * NY)
    first = s * count // (low // tile)
    for n in range(2):
        b = (first + n) % 10
        i = b % NY
        lh, ll = split(proj[:, lanes(i, side)].T)
        rh, rl = split(proj[:, lanes((i + b // NY) % NY, side)])
        block[pl.ds(n * side, side), :] = product(lh, ll, rh, rl)
    for n in range(count):
        at = s * count + n
        row = (at // (low // tile) - first) * side + core * low + at % (low // tile) * tile
        own_piece[pl.ds(n * tile, tile), :] = block[pl.ds(pl.multiple_of(row, tile), tile), :]
    size = count * tile
    zland[lanes(z, size), :] = own_piece[...]

    def to_z(k, _):
        pltpu.make_async_remote_copy(
            src_ref=own_piece, dst_ref=zland.at[lanes(z, size), :],
            send_sem=z_send, recv_sem=z_recv, device_id=z_peer(k), device_id_type=MESH,
        ).start()
        return 0

    lax.fori_loop(1, NZ, to_z, 0)
    view = zland.at[pl.ds(0, (NZ - 1) * size), :]
    z_all = pltpu.make_async_remote_copy(
        src_ref=view, dst_ref=view, send_sem=z_send, recv_sem=z_recv,
        device_id=z_peer(1), device_id_type=MESH,
    )
    z_all.wait_recv()
    total = zland[pl.ds(0, size), :]
    for k in range(1, NZ):
        total = total + zland[pl.ds(k * size, size), :]

    def packed_rows(of_core, of_y, of_x, chips):
        return pl.ds(pl.multiple_of(((of_core * NY + of_y) * NX + of_x) * size, size), chips * size)

    mine = packed_rows(core, y, x, 1)
    packed[mine, :] = total
    for k in range(1, NX * NY):
        kx, ky = k % NX, k // NX
        r2 = ((x + kx) % NX) * 2 + core
        pltpu.make_async_remote_copy(
            src_ref=packed.at[mine, :], dst_ref=packed.at[mine, :],
            send_sem=g_send, recv_sem=g_recv.at[ky],
            device_id=(r2, ((y + ky) % NY) * NZ + z), device_id_type=MESH,
        ).start()
    partner = (x * 2 + 1 - core, c)
    crossings = []
    for ky in range(NY):
        y2 = (y - ky + NY) % NY
        view = packed.at[pl.ds(0, (NX - 1 if ky == 0 else NX) * size), :]
        pltpu.make_async_remote_copy(
            src_ref=view, dst_ref=view, send_sem=g_send, recv_sem=g_recv.at[ky],
            device_id=partner, device_id_type=MESH,
        ).wait_recv()
        at = packed_rows(core, y2, 0, NX)
        copy = pltpu.make_async_remote_copy(
            src_ref=packed.at[at, :], dst_ref=packed.at[at, :],
            send_sem=d_send.at[ky], recv_sem=d_recv.at[ky],
            device_id=partner, device_id_type=MESH,
        )
        copy.start()
        crossings.append(copy)
    for ky in range(NY):
        at = packed_rows(1 - core, (y - ky + NY) % NY, 0, NX)
        pltpu.make_async_remote_copy(
            src_ref=packed.at[at, :], dst_ref=packed.at[at, :],
            send_sem=d_send.at[ky], recv_sem=d_recv.at[ky],
            device_id=partner, device_id_type=MESH,
        ).wait_recv()

    squares = jnp.zeros((low, side), F32)
    for b in range(10):
        o, i = b // NY, b % NY
        j = (i + o) % NY
        for h in range(2):
            part_of = packed[pl.ds((h * 10 + b) * low, low), :]
            squares = squares + (1.0 if o == 0 else 2.0) * (part_of * part_of)
            t[pl.ds(i * side + h * low, low), pl.ds(j * side, side)] = part_of
        if o:
            t[pl.ds(j * side, side), pl.ds(i * side, side)] = t[
                pl.ds(i * side, side), pl.ds(j * side, side)
            ].T
    scale = jnp.sqrt(jnp.full((1, 1), jnp.sum(squares), F32) + 1e-06)
    root_scale = jnp.sqrt(scale)
    t[...] = t[...] / scale

    wide_len, col_len = root.shape[1], root.shape[0]
    v[pl.ds(0, cols), :] = proj[lanes(y, cols), :]
    v[pl.ds(cols, col_len), :] = t[lanes(c, col_len), :]

    def split_t():
        hi, lo = split(t[...])
        t_hi[...] = hi
        t_lo[...] = lo

    def advance():
        vh, vl = split(v[...])
        v[...] = 1.5 * v[...] - 0.5 * product(vh, vl, t_hi[...], t_lo[...])

    def step(_, carry):
        split_t()
        advance()
        b = product(t_hi[...], t_lo[...], t_hi[...], t_lo[...])
        hi, lo = split(b)
        b_hi[...] = hi
        b_lo[...] = lo
        t[...] = (2.25 * t[...] - 1.5 * b) + 0.25 * product(
            b_hi[...], b_lo[...], t_hi[...], t_lo[...]
        )
        return carry

    lax.fori_loop(0, ITERS - 1, step, 0)
    split_t()
    advance()
    right[...] = v[pl.ds(0, cols), :] / root_scale
    ours = v[pl.ds(cols, col_len), :] * root_scale
    turn = (width - r * wide_len) % width
    root[...] = pltpu.roll(ours, turn, 1)[:, :wide_len]

    for copy in copies + crossings:
        copy.wait_send()
    for k in range(1, NY):
        y_copy(k).wait_send()
    for pair in (0, 1):
        all_of(land, pair, p_send, p_recv).wait_send()
        all_of(proj, pair, a_send, a_recv).wait_send()
    z_all.wait_send()
    view = zland.at[pl.ds(0, size), :]
    for k in range(1, NX * NY):
        pltpu.make_async_remote_copy(
            src_ref=view, dst_ref=view, send_sem=g_send, recv_sem=g_recv.at[0],
            device_id=partner, device_id_type=MESH,
        ).wait_send()


def local(matrix, basis):
    cols, depth = matrix.shape
    rows, width = basis.shape
    part = depth // NY
    side = width // NY
    size = 10 * side // (2 * NX * NY)
    row_len, col_len = width // NR, width // (NY * NZ)
    dma = pltpu.SemaphoreType.DMA
    vmem = pl.BlockSpec(memory_space=pltpu.VMEM)
    hbm = pl.BlockSpec(memory_space=pltpu.HBM)
    root, right = pl.pallas_call(
        step_kernel,
        name="step",
        out_shape=(
            jax.ShapeDtypeStruct((col_len, row_len), F32),
            jax.ShapeDtypeStruct((cols, width), F32),
        ),
        in_specs=[hbm, hbm],
        out_specs=(vmem, vmem),
        scratch_shapes=[
            pltpu.VMEM((cols, depth), F32),
            pltpu.VMEM((NY * cols, part), F32),
            pltpu.VMEM((NY * cols, part), BF16),
            pltpu.VMEM((NY * cols, part), BF16),
            pltpu.VMEM((NZ * rows, width), F32),
            pltpu.VMEM((NY * cols, width), F32),
            pltpu.VMEM(((PLANE - 1) * cols // NR, width), F32),
            pltpu.VMEM((NY * cols, width), F32),
            pltpu.VMEM((2 * side, side), F32),
            pltpu.VMEM((size, side), F32),
            pltpu.VMEM((NZ * size, side), F32),
            pltpu.VMEM((PLANE * size, side), F32),
            pltpu.VMEM((width, width), F32),
            pltpu.VMEM((width, width), BF16),
            pltpu.VMEM((width, width), BF16),
            pltpu.VMEM((width, width), BF16),
            pltpu.VMEM((width, width), BF16),
            pltpu.VMEM((cols + col_len, width), F32),
            dma((NY - 1,)), dma((NY - 1,)),
            dma((4, 4)), dma((4, 4)), dma((4, 4)), dma((4, 4)), dma((2,)),
            dma((2,)), dma((2,)), dma((2,)), dma((2,)),
            dma, dma, dma, dma((NY,)), dma((NY,)), dma((NY,)),
        ],
        compiler_params=pltpu.CompilerParams(
            collective_id=0, has_side_effects=True, vmem_limit_bytes=60 * 2**20
        ),
    )(matrix, basis)
    return root.T, right


def solution(mesh):
    return jax.shard_map(
        local,
        mesh=mesh,
        in_specs=(P("col", "row"), P(("row", "col"), None)),
        out_specs=(P("row", "col"), P("col", None)),
        check_vma=False,
    )
```

```python
import functools

import jax
import jax.numpy as jnp
from jax import lax
from jax.experimental import pallas as pl
from jax.experimental.pallas import tpu as pltpu
from jax.sharding import PartitionSpec as P

MESH = pl.DeviceIdType.MESH
ITERS = 8
F32 = jnp.float32
BF16 = jnp.bfloat16
NX, NY, NZ = 4, 4, 8
NR, PLANE = 2 * NX, 2 * NX * NY


def split(a):
    hi = a.astype(BF16)
    return hi, (a - hi.astype(F32)).astype(BF16)


def product(ah, al, bh, bl, dims=(((1,), (0,)), ((), ()))):
    dot = functools.partial(
        lax.dot_general, dimension_numbers=dims, preferred_element_type=F32
    )
    return dot(ah, bh) + (dot(ah, bl) + dot(al, bh))


PEERS = sorted(
    [(dx, dy, dc) for dx in range(NX) for dy in range(NY) for dc in range(2)][1:],
    key=lambda p: -(min(p[0], NX - p[0]) * 2 + min(p[1], NY - p[1]) * 2 + p[2]),
)
Z_STEPS = sorted(range(1, NZ), key=lambda d: -min(d, NZ - d))


def lanes(i, size):
    return pl.ds(pl.multiple_of(i * size, size), size)


def gather_kernel(
    mat_hbm, bas_hbm, packed, own_cols,
    mat, m_in, m_hi, m_lo, q, acc, land, proj, block, own_piece, zland,
    y_send, y_recv, f_send, f_recv, b_send, b_recv, local_sem,
    p_send, p_recv, a_send, a_recv, z_send, z_recv, g_send, g_recv, d_send, d_recv,
):
    r, c = lax.axis_index("row"), lax.axis_index("col")
    y, z = c // NZ, c % NZ
    x, core = r // 2, r % 2
    cols = mat.shape[0]
    part = mat.shape[1] // NY
    rows, width = bas_hbm.shape
    half = rows // 2
    wide = width // 4
    piece = cols // NR

    near_x = [(x + d) % NX for d in range(NX)]
    near_y = [(y + d) % NY for d in range(NY)]
    near_row = [[n * 2 + (core + d) % 2 for d in range(2)] for n in near_x]
    near_col = [n * NZ + z for n in near_y]

    def plane_peer(k):
        dx, dy, dc = PEERS[k]
        return near_row[dx][dc], near_y[dy], near_col[dy]

    def z_peer(k):
        return (r, y * NZ + (z + k) % NZ)

    own_basis = pltpu.make_async_copy(bas_hbm, q.at[lanes(z, rows), :], local_sem.at[0])
    own_basis.start()
    own_matrix = pltpu.make_async_copy(mat_hbm, mat, local_sem.at[1])
    own_matrix.start()

    barrier = pltpu.get_barrier_semaphore()

    for k in Z_STEPS:
        pl.semaphore_signal(barrier, inc=1, device_id=z_peer(k), device_id_type=MESH)
    for k in range(PLANE - 1):
        r2, _, c2 = plane_peer(k)
        pl.semaphore_signal(barrier, inc=1, device_id=(r2, c2), device_id_type=MESH)
    with jax.named_scope("barrier"):
        pl.semaphore_wait(barrier, PLANE - 1 + NZ - 1)

    def ring_copy(m, d, ahead):
        sign = 1 if ahead else -1
        owner = (z - sign * d + NZ) % NZ
        here = pl.ds(m * wide, wide)
        span = pl.ds(pl.multiple_of(owner * rows, rows), rows)
        if d == 3:
            start = owner * rows + (0 if ahead else half)
            span = pl.ds(pl.multiple_of(start, half), half)
        send, recv = (f_send, f_recv) if ahead else (b_send, b_recv)
        return pltpu.make_async_remote_copy(
            src_ref=q.at[span, here], dst_ref=q.at[span, here], send_sem=send.at[m, d], recv_sem=recv.at[m, d],
            device_id=(r, y * NZ + (z + sign + NZ) % NZ), device_id_type=MESH,
        )

    def ring_wait(m, d, ahead):
        sign = 1 if ahead else -1
        owner = (z - sign * (d + 1) + NZ) % NZ
        here = pl.ds(m * wide, wide)
        span = pl.ds(pl.multiple_of(owner * rows, rows), rows)
        if d == 3:
            start = owner * rows + (0 if ahead else half)
            span = pl.ds(pl.multiple_of(start, half), half)
        send, recv = (f_send, f_recv) if ahead else (b_send, b_recv)
        pltpu.make_async_remote_copy(
            src_ref=q.at[span, here], dst_ref=q.at[span, here],
            send_sem=send.at[m, d], recv_sem=recv.at[m, d],
            device_id=(r, y * NZ + (z + sign + NZ) % NZ), device_id_type=MESH,
        ).wait_recv()

    def y_copy(k):
        y2 = (y + k) % NY
        return pltpu.make_async_remote_copy(
            src_ref=mat.at[:, lanes(y2, part)], dst_ref=m_in.at[lanes(y, cols), :],
            send_sem=y_send.at[k - 1], recv_sem=y_recv.at[k - 1],
            device_id=(r, y2 * NZ + z), device_id_type=MESH,
        )

    def y_wait(k):
        src = (y - k + NY) % NY
        pltpu.make_async_remote_copy(
            src_ref=mat.at[:, lanes(src, part)], dst_ref=m_in.at[lanes(src, cols), :],
            send_sem=y_send.at[k - 1], recv_sem=y_recv.at[k - 1],
            device_id=(r, src * NZ + z), device_id_type=MESH,
        ).wait_recv()

    copies = []

    def issue(m, d):
        for ahead in (True, False):
            if d > 0:
                ring_wait(m, d - 1, ahead)
            copy = ring_copy(m, d, ahead)
            copy.start()
            copies.append(copy)

    def split_rows(src):
        def one(i, _):
            at = pl.ds(pl.multiple_of(i * 16, 16), 16)
            hi, lo = split(m_in[at, :])
            m_hi[at, :] = hi
            m_lo[at, :] = lo
            return 0

        lax.fori_loop(src * (cols // 16), (src + 1) * (cols // 16), one, 0)

    def own_split(i, _):
        hi, lo = split(mat[pl.ds(pl.multiple_of(i * 16, 16), 16), lanes(y, part)])
        at = pl.ds(pl.multiple_of(y * cols + i * 16, 16), 16)
        m_hi[at, :] = hi
        m_lo[at, :] = lo
        return 0

    def multiply(pair, first, last):
        here = pl.ds(pair * 2 * wide, 2 * wide)

        def one(o, _):
            owner = (z + o) % NZ
            qh, ql = split(q[lanes(owner, rows), here])
            at = lanes(owner, rows)
            acc[:, here] += product(m_hi[:, at], m_lo[:, at], qh, ql)
            return 0

        lax.fori_loop(first, last, one, 0)

    def spread_partial(pair):
        here = pl.ds(pair * 2 * wide, 2 * wide)

        for k in range(PLANE - 1):
            r2, y2, c2 = plane_peer(k)
            src = pl.ds(pl.multiple_of(y2 * cols + r2 * piece, piece), piece)
            pltpu.make_async_remote_copy(
                src_ref=acc.at[src, here], dst_ref=land.at[pl.ds(k * piece, piece), here],
                send_sem=p_send.at[pair], recv_sem=p_recv.at[pair],
                device_id=(r2, c2), device_id_type=MESH,
            ).start()

    mine = pl.ds(pl.multiple_of(y * cols + r * piece, piece), piece)

    def all_of(ref, pair, send, recv):
        here = pl.ds(pair * 2 * wide, 2 * wide)
        view = ref.at[pl.ds(0, (PLANE - 1) * piece), here]
        return pltpu.make_async_remote_copy(
            src_ref=view, dst_ref=view, send_sem=send.at[pair], recv_sem=recv.at[pair],
            device_id=z_peer(1), device_id_type=MESH,
        )

    def total_and_spread(pair):
        here = pl.ds(pair * 2 * wide, 2 * wide)
        all_of(land, pair, p_send, p_recv).wait_recv()
        total = acc[mine, here]
        for k in range(PLANE - 1):
            total = total + land[pl.ds(k * piece, piece), here]
        proj[mine, here] = total

        for k in range(PLANE - 1):
            r2, _, c2 = plane_peer(k)
            pltpu.make_async_remote_copy(
                src_ref=proj.at[mine, here], dst_ref=proj.at[mine, here],
                send_sem=a_send.at[pair], recv_sem=a_recv.at[pair],
                device_id=(r2, c2), device_id_type=MESH,
            ).start()

    own_basis.wait()
    issue(0, 0)
    own_matrix.wait()
    for k in range(1, NY):
        y_copy(k).start()
    issue(1, 0)
    acc[...] = jnp.zeros_like(acc)
    lax.fori_loop(0, cols // 16, own_split, 0)
    for d in range(1, 4):
        with jax.named_scope(f"issue_0{d}"):
            issue(0, d)
        with jax.named_scope(f"issue_1{d}"):
            issue(1, d)
    with jax.named_scope("issue_20"):
        issue(2, 0)
    with jax.named_scope("issue_30"):
        issue(3, 0)
    with jax.named_scope("issue_21"):
        issue(2, 1)
    with jax.named_scope("y_wait"):
        for k in range(1, NY):
            y_wait(k)
            split_rows((y - k + NY) % NY)
    for m in (0, 1):
        for ahead in (True, False):
            ring_wait(m, 3, ahead)
    with jax.named_scope("multiply_0"):
        multiply(0, 0, NZ)
    with jax.named_scope("spread_0"):
        spread_partial(0)
    with jax.named_scope("issue_31"):
        issue(3, 1)
    with jax.named_scope("issue_22"):
        issue(2, 2)
    with jax.named_scope("issue_32"):
        issue(3, 2)
    multiply(1, 0, 3)
    with jax.named_scope("issue_23"):
        issue(2, 3)
    with jax.named_scope("issue_33"):
        issue(3, 3)
    multiply(1, 3, 4)
    multiply(1, 5, NZ)
    with jax.named_scope("total_0"):
        total_and_spread(0)
    with jax.named_scope("last_wait"):
        for m in (2, 3):
            for ahead in (True, False):
                ring_wait(m, 3, ahead)
    with jax.named_scope("multiply_1d"):
        multiply(1, 4, 5)
    with jax.named_scope("spread_1"):
        spread_partial(1)
    with jax.named_scope("total_1"):
        total_and_spread(1)
    with jax.named_scope("proj_wait"):
        for pair in (0, 1):
            all_of(proj, pair, a_send, a_recv).wait_recv()

    side = width // NY
    low = side // 2
    tile = 8
    s = y * NX + x
    count = 10 * low // tile // (NX * NY)
    first = s * count // (low // tile)
    for n in range(2):
        b = (first + n) % 10
        i = b % NY
        lh, ll = split(proj[:, lanes(i, side)].T)
        rh, rl = split(proj[:, lanes((i + b // NY) % NY, side)])
        block[pl.ds(n * side, side), :] = product(lh, ll, rh, rl)
    for n in range(count):
        at = s * count + n
        row = (at // (low // tile) - first) * side + core * low + at % (low // tile) * tile
        own_piece[pl.ds(n * tile, tile), :] = block[pl.ds(pl.multiple_of(row, tile), tile), :]
    size = count * tile
    zland[lanes(z, size), :] = own_piece[...]

    for k in Z_STEPS:
        pltpu.make_async_remote_copy(
            src_ref=own_piece, dst_ref=zland.at[lanes(z, size), :],
            send_sem=z_send, recv_sem=z_recv, device_id=z_peer(k), device_id_type=MESH,
        ).start()
    view = zland.at[pl.ds(0, (NZ - 1) * size), :]
    z_all = pltpu.make_async_remote_copy(
        src_ref=view, dst_ref=view, send_sem=z_send, recv_sem=z_recv,
        device_id=z_peer(1), device_id_type=MESH,
    )
    with jax.named_scope("z_wait"):
        z_all.wait_recv()
    total = zland[pl.ds(0, size), :]
    for k in range(1, NZ):
        total = total + zland[pl.ds(k * size, size), :]

    def packed_rows(of_core, of_y, of_x, chips):
        return pl.ds(pl.multiple_of(((of_core * NY + of_y) * NX + of_x) * size, size), chips * size)

    mine = packed_rows(core, y, x, 1)
    packed[mine, :] = total
    for k in range(PLANE - 1):
        r2, _, c2 = plane_peer(k)
        if PEERS[k][2] == 0:
            pltpu.make_async_remote_copy(
                src_ref=packed.at[mine, :], dst_ref=packed.at[mine, :],
                send_sem=g_send, recv_sem=g_recv.at[PEERS[k][1]],
                device_id=(r2, c2), device_id_type=MESH,
            ).start()
    with jax.named_scope("gram_gather"):
        partner = (x * 2 + 1 - core, c)
        crossings = []
        for ky in range(NY):
            y2 = (y - ky + NY) % NY
            view = packed.at[pl.ds(0, (NX - 1 if ky == 0 else NX) * size), :]
            pltpu.make_async_remote_copy(
                src_ref=view, dst_ref=view, send_sem=g_send, recv_sem=g_recv.at[ky],
                device_id=partner, device_id_type=MESH,
            ).wait_recv()
            at = packed_rows(core, y2, 0, NX)
            copy = pltpu.make_async_remote_copy(
                src_ref=packed.at[at, :], dst_ref=packed.at[at, :],
                send_sem=d_send.at[ky], recv_sem=d_recv.at[ky],
                device_id=partner, device_id_type=MESH,
            )
            copy.start()
            crossings.append(copy)
        for ky in range(NY):
            at = packed_rows(1 - core, (y - ky + NY) % NY, 0, NX)
            pltpu.make_async_remote_copy(
                src_ref=packed.at[at, :], dst_ref=packed.at[at, :],
                send_sem=d_send.at[ky], recv_sem=d_recv.at[ky],
                device_id=partner, device_id_type=MESH,
            ).wait_recv()

    own_cols[...] = proj[lanes(y, cols), :]

    with jax.named_scope("send_waits"):
        for copy in copies + crossings:
            copy.wait_send()
        for k in range(1, NY):
            y_copy(k).wait_send()
        for pair in (0, 1):
            all_of(land, pair, p_send, p_recv).wait_send()
            all_of(proj, pair, a_send, a_recv).wait_send()
        z_all.wait_send()
        view = zland.at[pl.ds(0, size), :]
        for k in range(1, NX * NY):
            pltpu.make_async_remote_copy(
                src_ref=view, dst_ref=view, send_sem=g_send, recv_sem=g_recv.at[0],
                device_id=partner, device_id_type=MESH,
            ).wait_send()


def polar_kernel(packed, own_cols, root, right, t, u_hi, u_lo, b_hi, b_lo, v):
    r, c = lax.axis_index("row"), lax.axis_index("col")
    width = t.shape[0]
    cols = own_cols.shape[0]
    wide_len, col_len = root.shape[1], root.shape[0]
    side = width // NY
    low = side // 2
    squares = jnp.zeros((low, side), F32)
    for b in range(10):
        o, i = b // NY, b % NY
        j = (i + o) % NY
        for h in range(2):
            part_of = packed[pl.ds((h * 10 + b) * low, low), :]
            squares = squares + (1.0 if o == 0 else 2.0) * (part_of * part_of)
            t[pl.ds(i * side + h * low, low), pl.ds(j * side, side)] = part_of
        if o:
            t[pl.ds(j * side, side), pl.ds(i * side, side)] = t[
                pl.ds(i * side, side), pl.ds(j * side, side)
            ].T
    scale = jnp.sqrt(jnp.full((1, 1), jnp.sum(squares), F32) + 1e-06)
    root_scale = jnp.sqrt(scale)
    t[...] = t[...] / scale

    size = width // 2
    a, b, full = pl.ds(0, size), pl.ds(size, size), pl.ds(0, width)
    tail = pl.ds(width, cols + col_len)
    v[pl.ds(0, cols), :] = own_cols[...]
    v[pl.ds(cols, col_len), :] = t[lanes(c, col_len), :]

    def put(slot, rows, at, value):
        hi, lo = split(value)
        u_hi[slot, rows, at] = hi
        u_lo[slot, rows, at] = lo

    def put_b(rows, at, value):
        hi, lo = split(value)
        b_hi[rows, at] = hi
        b_lo[rows, at] = lo

    put(0, full, full, t[...])
    put(0, tail, full, v[...])
    for step in range(ITERS):
        now, new = step % 2, (step + 1) % 2

        def by_t(rows, at):
            return product(
                u_hi[now, rows, :], u_lo[now, rows, :], u_hi[now, full, at], u_lo[now, full, at]
            )

        def by_b(rows, at):
            return product(u_hi[now, rows, :], u_lo[now, rows, :], b_hi[full, at], b_lo[full, at])

        if step == ITERS - 1:
            v[...] = 1.5 * v[...] - 0.5 * by_t(tail, full)
            break
        value = by_t(a, a)
        put_b(a, a, value)
        t[a, a] = 2.25 * t[a, a] - 1.5 * value
        value = by_t(b, a)
        put_b(b, a, value)
        put_b(a, b, value.T)
        t[b, a] = 2.25 * t[b, a] - 1.5 * value
        value = by_t(b, b)
        left, right_half = by_t(tail, a), by_t(tail, b)
        put_b(b, b, value)
        t[b, b] = 2.25 * t[b, b] - 1.5 * value
        first, second = by_b(a, a), by_b(b, a)
        for at, moved in ((a, left), (b, right_half)):
            value = 1.5 * v[:, at] - 0.5 * moved
            v[:, at] = value
            put(new, tail, at, value)
        value = t[a, a] + 0.25 * first
        t[a, a] = value
        put(new, a, a, value)
        value = t[b, a] + 0.25 * second
        t[b, a] = value
        put(new, b, a, value)
        put(new, a, b, value.T)
        value = t[b, b] + 0.25 * by_b(b, b)
        t[b, b] = value
        put(new, b, b, value)
    right[...] = v[pl.ds(0, cols), :] / root_scale
    ours = v[pl.ds(cols, col_len), :] * root_scale
    turn = (width - r * wide_len) % width
    root[...] = pltpu.roll(ours, turn, 1)[:, :wide_len]


def local(matrix, basis):
    cols, depth = matrix.shape
    rows, width = basis.shape
    part = depth // NY
    side = width // NY
    size = 10 * side // (2 * NX * NY)
    row_len, col_len = width // NR, width // (NY * NZ)
    dma = pltpu.SemaphoreType.DMA
    vmem = pl.BlockSpec(memory_space=pltpu.VMEM)
    hbm = pl.BlockSpec(memory_space=pltpu.HBM)
    packed, own_cols = pl.pallas_call(
        gather_kernel,
        name="gather",
        out_shape=(
            jax.ShapeDtypeStruct((PLANE * size, side), F32),
            jax.ShapeDtypeStruct((cols, width), F32),
        ),
        in_specs=[hbm, hbm],
        out_specs=(vmem, vmem),
        scratch_shapes=[
            pltpu.VMEM((cols, depth), F32),
            pltpu.VMEM((NY * cols, part), F32),
            pltpu.VMEM((NY * cols, part), BF16),
            pltpu.VMEM((NY * cols, part), BF16),
            pltpu.VMEM((NZ * rows, width), F32),
            pltpu.VMEM((NY * cols, width), F32),
            pltpu.VMEM(((PLANE - 1) * cols // NR, width), F32),
            pltpu.VMEM((NY * cols, width), F32),
            pltpu.VMEM((2 * side, side), F32),
            pltpu.VMEM((size, side), F32),
            pltpu.VMEM((NZ * size, side), F32),
            dma((NY - 1,)), dma((NY - 1,)),
            dma((4, 4)), dma((4, 4)), dma((4, 4)), dma((4, 4)), dma((2,)),
            dma((2,)), dma((2,)), dma((2,)), dma((2,)),
            dma, dma, dma, dma((NY,)), dma((NY,)), dma((NY,)),
        ],
        compiler_params=pltpu.CompilerParams(
            collective_id=0, has_side_effects=True, vmem_limit_bytes=48 * 2**20
        ),
    )(*(pltpu.with_memory_space_constraint(a, pltpu.HBM) for a in (matrix, basis)))
    root, right = pl.pallas_call(
        polar_kernel,
        name="polar",
        out_shape=(
            jax.ShapeDtypeStruct((col_len, row_len), F32),
            jax.ShapeDtypeStruct((cols, width), F32),
        ),
        in_specs=[vmem, vmem],
        out_specs=(vmem, vmem),
        scratch_shapes=[
            pltpu.VMEM((width, width), F32),
            pltpu.VMEM((2, width + cols + col_len, width), BF16),
            pltpu.VMEM((2, width + cols + col_len, width), BF16),
            pltpu.VMEM((width, width), BF16),
            pltpu.VMEM((width, width), BF16),
            pltpu.VMEM((cols + col_len, width), F32),
        ],
        compiler_params=pltpu.CompilerParams(vmem_limit_bytes=24 * 2**20),
    )(packed, own_cols)
    return root.T, right


def solution(mesh):
    return jax.shard_map(
        local,
        mesh=mesh,
        in_specs=(P("col", "row"), P(("row", "col"), None)),
        out_specs=(P("row", "col"), P("col", None)),
        check_vma=False,
    )
```

```python
import functools

import jax
import jax.numpy as jnp
from jax import lax
from jax.experimental import pallas as pl
from jax.experimental.pallas import tpu as pltpu
from jax.sharding import PartitionSpec as P

MESH = pl.DeviceIdType.MESH
ITERS = 8
F32 = jnp.float32
BF16 = jnp.bfloat16
NX, NY, NZ = 4, 4, 8
NR, PLANE = 2 * NX, 2 * NX * NY


def split(a):
    hi = a.astype(BF16)
    return hi, (a - hi.astype(F32)).astype(BF16)


def product(ah, al, bh, bl, dims=(((1,), (0,)), ((), ()))):
    dot = functools.partial(
        lax.dot_general, dimension_numbers=dims, preferred_element_type=F32
    )
    return dot(ah, bh) + (dot(ah, bl) + dot(al, bh))


PEERS = sorted(
    [(dx, dy, dc) for dx in range(NX) for dy in range(NY) for dc in range(2)][1:],
    key=lambda p: -(min(p[0], NX - p[0]) * 2 + min(p[1], NY - p[1]) * 2 + p[2]),
)
Z_STEPS = sorted(range(1, NZ), key=lambda d: -min(d, NZ - d))


def lanes(i, size):
    return pl.ds(pl.multiple_of(i * size, size), size)


def gather_kernel(
    mat_hbm, bas_hbm, packed, own_cols,
    mat, m_in, m_hi, m_lo, q, acc, land, proj, block, own_piece, zland,
    y_send, y_recv, f_send, f_recv, b_send, b_recv, local_sem,
    p_send, p_recv, a_send, a_recv, z_send, z_recv, g_send, g_recv, d_send, d_recv, plane_sem,
):
    r, c = lax.axis_index("row"), lax.axis_index("col")
    y, z = c // NZ, c % NZ
    x, core = r // 2, r % 2
    cols = mat.shape[0]
    part = mat.shape[1] // NY
    rows, width = bas_hbm.shape
    half = rows // 2
    wide = width // 4
    piece = cols // NR

    near_x = [(x + d) % NX for d in range(NX)]
    near_y = [(y + d) % NY for d in range(NY)]
    near_row = [[n * 2 + (core + d) % 2 for d in range(2)] for n in near_x]
    near_col = [n * NZ + z for n in near_y]

    def plane_peer(k):
        dx, dy, dc = PEERS[k]
        return near_row[dx][dc], near_y[dy], near_col[dy]

    def z_peer(k):
        return (r, y * NZ + (z + k) % NZ)

    own_basis = pltpu.make_async_copy(bas_hbm, q.at[lanes(z, rows), :], local_sem.at[0])
    own_basis.start()
    own_matrix = pltpu.make_async_copy(mat_hbm, mat, local_sem.at[1])
    own_matrix.start()

    barrier = pltpu.get_barrier_semaphore()

    near = [z_peer(1), z_peer(NZ - 1)] + [(r, near_col[d]) for d in range(1, NY)]
    for k in range(PLANE - 1):
        if PEERS[k][1] == 0:
            near.append((plane_peer(k)[0], c))
    for peer in near:
        pl.semaphore_signal(barrier, inc=1, device_id=peer, device_id_type=MESH)
    with jax.named_scope("barrier"):
        pl.semaphore_wait(barrier, len(near))
    for d in range(1, NY):
        pl.semaphore_signal(plane_sem, inc=1, device_id=(r, near_col[d]), device_id_type=MESH)

    def ring_copy(m, d, ahead):
        sign = 1 if ahead else -1
        owner = (z - sign * d + NZ) % NZ
        here = pl.ds(m * wide, wide)
        span = pl.ds(pl.multiple_of(owner * rows, rows), rows)
        if d == 3:
            start = owner * rows + (0 if ahead else half)
            span = pl.ds(pl.multiple_of(start, half), half)
        send, recv = (f_send, f_recv) if ahead else (b_send, b_recv)
        return pltpu.make_async_remote_copy(
            src_ref=q.at[span, here], dst_ref=q.at[span, here], send_sem=send.at[m, d], recv_sem=recv.at[m, d],
            device_id=(r, y * NZ + (z + sign + NZ) % NZ), device_id_type=MESH,
        )

    def ring_wait(m, d, ahead):
        sign = 1 if ahead else -1
        owner = (z - sign * (d + 1) + NZ) % NZ
        here = pl.ds(m * wide, wide)
        span = pl.ds(pl.multiple_of(owner * rows, rows), rows)
        if d == 3:
            start = owner * rows + (0 if ahead else half)
            span = pl.ds(pl.multiple_of(start, half), half)
        send, recv = (f_send, f_recv) if ahead else (b_send, b_recv)
        pltpu.make_async_remote_copy(
            src_ref=q.at[span, here], dst_ref=q.at[span, here],
            send_sem=send.at[m, d], recv_sem=recv.at[m, d],
            device_id=(r, y * NZ + (z + sign + NZ) % NZ), device_id_type=MESH,
        ).wait_recv()

    def y_copy(k):
        y2 = (y + k) % NY
        return pltpu.make_async_remote_copy(
            src_ref=mat.at[:, lanes(y2, part)], dst_ref=m_in.at[lanes(y, cols), :],
            send_sem=y_send.at[k - 1], recv_sem=y_recv.at[k - 1],
            device_id=(r, y2 * NZ + z), device_id_type=MESH,
        )

    def y_wait(k):
        src = (y - k + NY) % NY
        pltpu.make_async_remote_copy(
            src_ref=mat.at[:, lanes(src, part)], dst_ref=m_in.at[lanes(src, cols), :],
            send_sem=y_send.at[k - 1], recv_sem=y_recv.at[k - 1],
            device_id=(r, src * NZ + z), device_id_type=MESH,
        ).wait_recv()

    copies = []

    def issue(m, d):
        for ahead in (True, False):
            if d > 0:
                ring_wait(m, d - 1, ahead)
            copy = ring_copy(m, d, ahead)
            copy.start()
            copies.append(copy)

    def split_rows(src):
        def one(i, _):
            at = pl.ds(pl.multiple_of(i * 16, 16), 16)
            hi, lo = split(m_in[at, :])
            m_hi[at, :] = hi
            m_lo[at, :] = lo
            return 0

        lax.fori_loop(src * (cols // 16), (src + 1) * (cols // 16), one, 0)

    def own_split(i, _):
        hi, lo = split(mat[pl.ds(pl.multiple_of(i * 16, 16), 16), lanes(y, part)])
        at = pl.ds(pl.multiple_of(y * cols + i * 16, 16), 16)
        m_hi[at, :] = hi
        m_lo[at, :] = lo
        return 0

    groups = [pl.ds(0, 2 * wide), pl.ds(2 * wide, wide), pl.ds(3 * wide, wide)]
    late = pl.ds(2 * wide, 2 * wide)

    def multiply(here, first, last):

        def one(o, _):
            owner = (z + o) % NZ
            qh, ql = split(q[lanes(owner, rows), here])
            at = lanes(owner, rows)
            acc[:, here] += product(m_hi[:, at], m_lo[:, at], qh, ql)
            return 0

        lax.fori_loop(first, last, one, 0)

    def spread_partial(group):
        here = groups[group]

        for k in range(PLANE - 1):
            r2, y2, c2 = plane_peer(k)
            src = pl.ds(pl.multiple_of(y2 * cols + r2 * piece, piece), piece)
            pltpu.make_async_remote_copy(
                src_ref=acc.at[src, here], dst_ref=land.at[pl.ds(k * piece, piece), here],
                send_sem=p_send.at[group], recv_sem=p_recv.at[group],
                device_id=(r2, c2), device_id_type=MESH,
            ).start()

    mine = pl.ds(pl.multiple_of(y * cols + r * piece, piece), piece)

    def all_of(ref, group, send, recv):
        view = ref.at[pl.ds(0, (PLANE - 1) * piece), groups[group]]
        return pltpu.make_async_remote_copy(
            src_ref=view, dst_ref=view, send_sem=send.at[group], recv_sem=recv.at[group],
            device_id=z_peer(1), device_id_type=MESH,
        )

    def total_and_spread(group):
        here = groups[group]
        all_of(land, group, p_send, p_recv).wait_recv()
        total = acc[mine, here]
        for k in range(PLANE - 1):
            total = total + land[pl.ds(k * piece, piece), here]
        proj[mine, here] = total

        for k in range(PLANE - 1):
            r2, _, c2 = plane_peer(k)
            pltpu.make_async_remote_copy(
                src_ref=proj.at[mine, here], dst_ref=proj.at[mine, here],
                send_sem=a_send.at[group], recv_sem=a_recv.at[group],
                device_id=(r2, c2), device_id_type=MESH,
            ).start()

    own_basis.wait()
    issue(0, 0)
    own_matrix.wait()
    for k in range(1, NY):
        y_copy(k).start()
    issue(1, 0)
    acc[...] = jnp.zeros_like(acc)
    lax.fori_loop(0, cols // 16, own_split, 0)
    for d in range(1, 4):
        with jax.named_scope(f"issue_0{d}"):
            issue(0, d)
        with jax.named_scope(f"issue_1{d}"):
            issue(1, d)
    with jax.named_scope("issue_20"):
        issue(2, 0)
    with jax.named_scope("issue_30"):
        issue(3, 0)
    with jax.named_scope("issue_21"):
        issue(2, 1)
    with jax.named_scope("y_wait"):
        for k in range(1, NY):
            y_wait(k)
            split_rows((y - k + NY) % NY)
    for m in (0, 1):
        for ahead in (True, False):
            ring_wait(m, 3, ahead)
    with jax.named_scope("multiply_0"):
        multiply(groups[0], 0, NZ)
    with jax.named_scope("spread_0"):
        pl.semaphore_wait(plane_sem, NY - 1)
        spread_partial(0)
    with jax.named_scope("issue_31"):
        issue(3, 1)
    with jax.named_scope("issue_22"):
        issue(2, 2)
    with jax.named_scope("issue_32"):
        issue(3, 2)
    multiply(late, 0, 3)
    with jax.named_scope("issue_23"):
        issue(2, 3)
    with jax.named_scope("issue_33"):
        issue(3, 3)
    multiply(late, 3, 4)
    multiply(late, 5, NZ)
    with jax.named_scope("total_0"):
        total_and_spread(0)
    for m in (2, 3):
        with jax.named_scope("last_wait"):
            for ahead in (True, False):
                ring_wait(m, 3, ahead)
        with jax.named_scope("multiply_last"):
            multiply(groups[m - 1], 4, 5)
        with jax.named_scope("spread_last"):
            spread_partial(m - 1)
    with jax.named_scope("total_1"):
        total_and_spread(1)
    with jax.named_scope("total_2"):
        total_and_spread(2)
    with jax.named_scope("proj_wait"):
        for group in range(3):
            all_of(proj, group, a_send, a_recv).wait_recv()

    side = width // NY
    low = side // 2
    tile = 8
    s = y * NX + x
    count = 10 * low // tile // (NX * NY)
    first = s * count // (low // tile)
    for n in range(2):
        b = (first + n) % 10
        i = b % NY
        lh, ll = split(proj[:, lanes(i, side)].T)
        rh, rl = split(proj[:, lanes((i + b // NY) % NY, side)])
        block[pl.ds(n * side, side), :] = product(lh, ll, rh, rl)
    for n in range(count):
        at = s * count + n
        row = (at // (low // tile) - first) * side + core * low + at % (low // tile) * tile
        own_piece[pl.ds(n * tile, tile), :] = block[pl.ds(pl.multiple_of(row, tile), tile), :]
    size = count * tile
    zland[lanes(z, size), :] = own_piece[...]

    for k in Z_STEPS:
        pltpu.make_async_remote_copy(
            src_ref=own_piece, dst_ref=zland.at[lanes(z, size), :],
            send_sem=z_send, recv_sem=z_recv, device_id=z_peer(k), device_id_type=MESH,
        ).start()
    view = zland.at[pl.ds(0, (NZ - 1) * size), :]
    z_all = pltpu.make_async_remote_copy(
        src_ref=view, dst_ref=view, send_sem=z_send, recv_sem=z_recv,
        device_id=z_peer(1), device_id_type=MESH,
    )
    with jax.named_scope("z_wait"):
        z_all.wait_recv()
    total = zland[pl.ds(0, size), :]
    for k in range(1, NZ):
        total = total + zland[pl.ds(k * size, size), :]

    def packed_rows(of_core, of_y, of_x, chips):
        return pl.ds(pl.multiple_of(((of_core * NY + of_y) * NX + of_x) * size, size), chips * size)

    mine = packed_rows(core, y, x, 1)
    packed[mine, :] = total
    for k in range(PLANE - 1):
        r2, _, c2 = plane_peer(k)
        if PEERS[k][2] == 0:
            pltpu.make_async_remote_copy(
                src_ref=packed.at[mine, :], dst_ref=packed.at[mine, :],
                send_sem=g_send, recv_sem=g_recv.at[PEERS[k][1]],
                device_id=(r2, c2), device_id_type=MESH,
            ).start()
    with jax.named_scope("gram_gather"):
        partner = (x * 2 + 1 - core, c)
        crossings = []
        for ky in range(NY):
            y2 = (y - ky + NY) % NY
            view = packed.at[pl.ds(0, (NX - 1 if ky == 0 else NX) * size), :]
            pltpu.make_async_remote_copy(
                src_ref=view, dst_ref=view, send_sem=g_send, recv_sem=g_recv.at[ky],
                device_id=partner, device_id_type=MESH,
            ).wait_recv()
            at = packed_rows(core, y2, 0, NX)
            copy = pltpu.make_async_remote_copy(
                src_ref=packed.at[at, :], dst_ref=packed.at[at, :],
                send_sem=d_send.at[ky], recv_sem=d_recv.at[ky],
                device_id=partner, device_id_type=MESH,
            )
            copy.start()
            crossings.append(copy)
        for ky in range(NY):
            at = packed_rows(1 - core, (y - ky + NY) % NY, 0, NX)
            pltpu.make_async_remote_copy(
                src_ref=packed.at[at, :], dst_ref=packed.at[at, :],
                send_sem=d_send.at[ky], recv_sem=d_recv.at[ky],
                device_id=partner, device_id_type=MESH,
            ).wait_recv()

    own_cols[...] = proj[lanes(y, cols), :]

    with jax.named_scope("send_waits"):
        for copy in copies + crossings:
            copy.wait_send()
        for k in range(1, NY):
            y_copy(k).wait_send()
        for group in range(3):
            all_of(land, group, p_send, p_recv).wait_send()
            all_of(proj, group, a_send, a_recv).wait_send()
        z_all.wait_send()
        view = zland.at[pl.ds(0, size), :]
        for k in range(1, NX * NY):
            pltpu.make_async_remote_copy(
                src_ref=view, dst_ref=view, send_sem=g_send, recv_sem=g_recv.at[0],
                device_id=partner, device_id_type=MESH,
            ).wait_send()


def polar_kernel(packed, own_cols, root, right, t, u_hi, u_lo, b_hi, b_lo, v):
    r, c = lax.axis_index("row"), lax.axis_index("col")
    width = t.shape[0]
    cols = own_cols.shape[0]
    wide_len, col_len = root.shape[1], root.shape[0]
    side = width // NY
    low = side // 2
    squares = jnp.zeros((low, side), F32)
    for b in range(10):
        o, i = b // NY, b % NY
        j = (i + o) % NY
        for h in range(2):
            part_of = packed[pl.ds((h * 10 + b) * low, low), :]
            squares = squares + (1.0 if o == 0 else 2.0) * (part_of * part_of)
            t[pl.ds(i * side + h * low, low), pl.ds(j * side, side)] = part_of
        if o:
            t[pl.ds(j * side, side), pl.ds(i * side, side)] = t[
                pl.ds(i * side, side), pl.ds(j * side, side)
            ].T
    scale = jnp.sqrt(jnp.full((1, 1), jnp.sum(squares), F32) + 1e-06)
    root_scale = jnp.sqrt(scale)
    t[...] = t[...] / scale

    size = width // 2
    a, b, full = pl.ds(0, size), pl.ds(size, size), pl.ds(0, width)
    tail = pl.ds(width, cols + col_len)
    v[pl.ds(0, cols), :] = own_cols[...]
    v[pl.ds(cols, col_len), :] = t[lanes(c, col_len), :]

    def put(slot, rows, at, value):
        hi, lo = split(value)
        u_hi[slot, rows, at] = hi
        u_lo[slot, rows, at] = lo

    def put_b(rows, at, value):
        hi, lo = split(value)
        b_hi[rows, at] = hi
        b_lo[rows, at] = lo

    put(0, full, full, t[...])
    put(0, tail, full, v[...])
    for step in range(ITERS - 1):
        now, new = step % 2, (step + 1) % 2

        def by_t(rows, at):
            return product(
                u_hi[now, rows, :], u_lo[now, rows, :], u_hi[now, full, at], u_lo[now, full, at]
            )

        def by_b(rows, at):
            return product(u_hi[now, rows, :], u_lo[now, rows, :], b_hi[full, at], b_lo[full, at])

        if step == ITERS - 2:
            def times_t(value):
                hi, lo = split(value)
                both = jnp.concatenate([hi, lo], axis=0)
                dot = functools.partial(jnp.dot, preferred_element_type=F32)
                wide = dot(both, u_hi[now, full, :])
                rows = value.shape[0]
                return (wide[:rows] + wide[rows:]) + dot(hi, u_lo[now, full, :])

            def times_s(value):
                return 1.5 * value - 0.5 * times_t(value)

            value = times_s(v[...])
            v[...] = 1.5 * value - 0.5 * times_s(times_s(times_t(value)))
            break
        value = by_t(a, a)
        put_b(a, a, value)
        t[a, a] = 2.25 * t[a, a] - 1.5 * value
        value = by_t(b, a)
        put_b(b, a, value)
        put_b(a, b, value.T)
        t[b, a] = 2.25 * t[b, a] - 1.5 * value
        value = by_t(b, b)
        left, right_half = by_t(tail, a), by_t(tail, b)
        put_b(b, b, value)
        t[b, b] = 2.25 * t[b, b] - 1.5 * value
        first, second = by_b(a, a), by_b(b, a)
        for at, moved in ((a, left), (b, right_half)):
            value = 1.5 * v[:, at] - 0.5 * moved
            v[:, at] = value
            put(new, tail, at, value)
        value = t[a, a] + 0.25 * first
        t[a, a] = value
        put(new, a, a, value)
        value = t[b, a] + 0.25 * second
        t[b, a] = value
        put(new, b, a, value)
        put(new, a, b, value.T)
        value = t[b, b] + 0.25 * by_b(b, b)
        t[b, b] = value
        put(new, b, b, value)
    right[...] = v[pl.ds(0, cols), :] / root_scale
    ours = v[pl.ds(cols, col_len), :] * root_scale
    turn = (width - r * wide_len) % width
    root[...] = pltpu.roll(ours, turn, 1)[:, :wide_len]


def local(matrix, basis):
    cols, depth = matrix.shape
    rows, width = basis.shape
    part = depth // NY
    side = width // NY
    size = 10 * side // (2 * NX * NY)
    row_len, col_len = width // NR, width // (NY * NZ)
    dma = pltpu.SemaphoreType.DMA
    vmem = pl.BlockSpec(memory_space=pltpu.VMEM)
    hbm = pl.BlockSpec(memory_space=pltpu.HBM)
    packed, own_cols = pl.pallas_call(
        gather_kernel,
        name="gather",
        out_shape=(
            jax.ShapeDtypeStruct((PLANE * size, side), F32),
            jax.ShapeDtypeStruct((cols, width), F32),
        ),
        in_specs=[hbm, hbm],
        out_specs=(vmem, vmem),
        scratch_shapes=[
            pltpu.VMEM((cols, depth), F32),
            pltpu.VMEM((NY * cols, part), F32),
            pltpu.VMEM((NY * cols, part), BF16),
            pltpu.VMEM((NY * cols, part), BF16),
            pltpu.VMEM((NZ * rows, width), F32),
            pltpu.VMEM((NY * cols, width), F32),
            pltpu.VMEM(((PLANE - 1) * cols // NR, width), F32),
            pltpu.VMEM((NY * cols, width), F32),
            pltpu.VMEM((2 * side, side), F32),
            pltpu.VMEM((size, side), F32),
            pltpu.VMEM((NZ * size, side), F32),
            dma((NY - 1,)), dma((NY - 1,)),
            dma((4, 4)), dma((4, 4)), dma((4, 4)), dma((4, 4)), dma((2,)),
            dma((3,)), dma((3,)), dma((3,)), dma((3,)),
            dma, dma, dma, dma((NY,)), dma((NY,)), dma((NY,)),
            pltpu.SemaphoreType.REGULAR,
        ],
        compiler_params=pltpu.CompilerParams(
            collective_id=0, has_side_effects=True, vmem_limit_bytes=48 * 2**20
        ),
    )(*(pltpu.with_memory_space_constraint(a, pltpu.HBM) for a in (matrix, basis)))
    root, right = pl.pallas_call(
        polar_kernel,
        name="polar",
        out_shape=(
            jax.ShapeDtypeStruct((col_len, row_len), F32),
            jax.ShapeDtypeStruct((cols, width), F32),
        ),
        in_specs=[vmem, vmem],
        out_specs=(vmem, vmem),
        scratch_shapes=[
            pltpu.VMEM((width, width), F32),
            pltpu.VMEM((2, width + cols + col_len, width), BF16),
            pltpu.VMEM((2, width + cols + col_len, width), BF16),
            pltpu.VMEM((width, width), BF16),
            pltpu.VMEM((width, width), BF16),
            pltpu.VMEM((cols + col_len, width), F32),
        ],
        compiler_params=pltpu.CompilerParams(vmem_limit_bytes=24 * 2**20),
    )(packed, own_cols)
    return root.T, right


def solution(mesh):
    return jax.shard_map(
        local,
        mesh=mesh,
        in_specs=(P("col", "row"), P(("row", "col"), None)),
        out_specs=(P("row", "col"), P("col", None)),
        check_vma=False,
    )
```

```python
import functools

import jax
import jax.numpy as jnp
from jax import lax
from jax.experimental import pallas as pl
from jax.experimental.pallas import tpu as pltpu
from jax.sharding import PartitionSpec as P

MESH = pl.DeviceIdType.MESH
ITERS = 8
F32 = jnp.float32
BF16 = jnp.bfloat16
NX, NY, NZ = 4, 4, 8
NR, PLANE = 2 * NX, 2 * NX * NY


def split(a):
    hi = a.astype(BF16)
    return hi, (a - hi.astype(F32)).astype(BF16)


def product(ah, al, bh, bl, dims=(((1,), (0,)), ((), ()))):
    dot = functools.partial(
        lax.dot_general, dimension_numbers=dims, preferred_element_type=F32
    )
    return dot(ah, bh) + (dot(ah, bl) + dot(al, bh))


PEERS = sorted(
    [(dx, dy, dc) for dx in range(NX) for dy in range(NY) for dc in range(2)][1:],
    key=lambda p: -(min(p[0], NX - p[0]) * 2 + min(p[1], NY - p[1]) * 2 + p[2]),
)
Z_STEPS = sorted(range(1, NZ), key=lambda d: -min(d, NZ - d))


def lanes(i, size):
    return pl.ds(pl.multiple_of(i * size, size), size)


def gather_kernel(
    mat_hbm, bas_hbm, packed_early, packed_late, own_cols,
    mat, m_in, m_hi, m_lo, q, acc, land, proj, block,
    piece_early, piece_late, zland_early, zland_late,
    y_send, y_recv, f_send, f_recv, b_send, b_recv, local_sem,
    p_send, p_recv, a_send, a_recv, z_send, z_recv, g_send, g_recv, d_send, d_recv, plane_sem,
):
    r, c = lax.axis_index("row"), lax.axis_index("col")
    y, z = c // NZ, c % NZ
    x, core = r // 2, r % 2
    cols = mat.shape[0]
    part = mat.shape[1] // NY
    rows, width = bas_hbm.shape
    half = rows // 2
    wide = width // 4
    piece = cols // NR

    near_x = [(x + d) % NX for d in range(NX)]
    near_y = [(y + d) % NY for d in range(NY)]
    near_row = [[n * 2 + (core + d) % 2 for d in range(2)] for n in near_x]
    near_col = [n * NZ + z for n in near_y]

    def plane_peer(k):
        dx, dy, dc = PEERS[k]
        return near_row[dx][dc], near_y[dy], near_col[dy]

    def z_peer(k):
        return (r, y * NZ + (z + k) % NZ)

    own_basis = pltpu.make_async_copy(bas_hbm, q.at[lanes(z, rows), :], local_sem.at[0])
    own_basis.start()
    own_matrix = pltpu.make_async_copy(mat_hbm, mat, local_sem.at[1])
    own_matrix.start()

    barrier = pltpu.get_barrier_semaphore()

    near = [z_peer(1), z_peer(NZ - 1)] + [(r, near_col[d]) for d in range(1, NY)]
    for k in range(PLANE - 1):
        if PEERS[k][1] == 0:
            near.append((plane_peer(k)[0], c))
    for peer in near:
        pl.semaphore_signal(barrier, inc=1, device_id=peer, device_id_type=MESH)
    with jax.named_scope("barrier"):
        pl.semaphore_wait(barrier, len(near))
    for d in range(1, NY):
        pl.semaphore_signal(plane_sem, inc=1, device_id=(r, near_col[d]), device_id_type=MESH)

    def ring_copy(m, d, ahead):
        sign = 1 if ahead else -1
        owner = (z - sign * d + NZ) % NZ
        here = pl.ds(m * wide, wide)
        span = pl.ds(pl.multiple_of(owner * rows, rows), rows)
        if d == 3:
            start = owner * rows + (0 if ahead else half)
            span = pl.ds(pl.multiple_of(start, half), half)
        send, recv = (f_send, f_recv) if ahead else (b_send, b_recv)
        return pltpu.make_async_remote_copy(
            src_ref=q.at[span, here], dst_ref=q.at[span, here], send_sem=send.at[m, d], recv_sem=recv.at[m, d],
            device_id=(r, y * NZ + (z + sign + NZ) % NZ), device_id_type=MESH,
        )

    def ring_wait(m, d, ahead):
        sign = 1 if ahead else -1
        owner = (z - sign * (d + 1) + NZ) % NZ
        here = pl.ds(m * wide, wide)
        span = pl.ds(pl.multiple_of(owner * rows, rows), rows)
        if d == 3:
            start = owner * rows + (0 if ahead else half)
            span = pl.ds(pl.multiple_of(start, half), half)
        send, recv = (f_send, f_recv) if ahead else (b_send, b_recv)
        pltpu.make_async_remote_copy(
            src_ref=q.at[span, here], dst_ref=q.at[span, here],
            send_sem=send.at[m, d], recv_sem=recv.at[m, d],
            device_id=(r, y * NZ + (z + sign + NZ) % NZ), device_id_type=MESH,
        ).wait_recv()

    def y_copy(k):
        y2 = (y + k) % NY
        return pltpu.make_async_remote_copy(
            src_ref=mat.at[:, lanes(y2, part)], dst_ref=m_in.at[lanes(y, cols), :],
            send_sem=y_send.at[k - 1], recv_sem=y_recv.at[k - 1],
            device_id=(r, y2 * NZ + z), device_id_type=MESH,
        )

    def y_wait(k):
        src = (y - k + NY) % NY
        pltpu.make_async_remote_copy(
            src_ref=mat.at[:, lanes(src, part)], dst_ref=m_in.at[lanes(src, cols), :],
            send_sem=y_send.at[k - 1], recv_sem=y_recv.at[k - 1],
            device_id=(r, src * NZ + z), device_id_type=MESH,
        ).wait_recv()

    copies = []

    def issue(m, d):
        for ahead in (True, False):
            if d > 0:
                ring_wait(m, d - 1, ahead)
            copy = ring_copy(m, d, ahead)
            copy.start()
            copies.append(copy)

    def split_rows(src):
        def one(i, _):
            at = pl.ds(pl.multiple_of(i * 16, 16), 16)
            hi, lo = split(m_in[at, :])
            m_hi[at, :] = hi
            m_lo[at, :] = lo
            return 0

        lax.fori_loop(src * (cols // 16), (src + 1) * (cols // 16), one, 0)

    def own_split(i, _):
        hi, lo = split(mat[pl.ds(pl.multiple_of(i * 16, 16), 16), lanes(y, part)])
        at = pl.ds(pl.multiple_of(y * cols + i * 16, 16), 16)
        m_hi[at, :] = hi
        m_lo[at, :] = lo
        return 0

    groups = [pl.ds(0, 2 * wide), pl.ds(2 * wide, wide), pl.ds(3 * wide, wide)]
    late = pl.ds(2 * wide, 2 * wide)

    def multiply(here, first, last):

        def one(o, _):
            owner = (z + o) % NZ
            qh, ql = split(q[lanes(owner, rows), here])
            at = lanes(owner, rows)
            acc[:, here] += product(m_hi[:, at], m_lo[:, at], qh, ql)
            return 0

        lax.fori_loop(first, last, one, 0)

    def spread_partial(group):
        here = groups[group]

        for k in range(PLANE - 1):
            r2, y2, c2 = plane_peer(k)
            src = pl.ds(pl.multiple_of(y2 * cols + r2 * piece, piece), piece)
            pltpu.make_async_remote_copy(
                src_ref=acc.at[src, here], dst_ref=land.at[pl.ds(k * piece, piece), here],
                send_sem=p_send.at[group], recv_sem=p_recv.at[group],
                device_id=(r2, c2), device_id_type=MESH,
            ).start()

    mine = pl.ds(pl.multiple_of(y * cols + r * piece, piece), piece)

    def all_of(ref, group, send, recv):
        view = ref.at[pl.ds(0, (PLANE - 1) * piece), groups[group]]
        return pltpu.make_async_remote_copy(
            src_ref=view, dst_ref=view, send_sem=send.at[group], recv_sem=recv.at[group],
            device_id=z_peer(1), device_id_type=MESH,
        )

    def total_and_spread(group):
        here = groups[group]
        all_of(land, group, p_send, p_recv).wait_recv()
        total = acc[mine, here]
        for k in range(PLANE - 1):
            total = total + land[pl.ds(k * piece, piece), here]
        proj[mine, here] = total

        for k in range(PLANE - 1):
            r2, _, c2 = plane_peer(k)
            pltpu.make_async_remote_copy(
                src_ref=proj.at[mine, here], dst_ref=proj.at[mine, here],
                send_sem=a_send.at[group], recv_sem=a_recv.at[group],
                device_id=(r2, c2), device_id_type=MESH,
            ).start()

    own_basis.wait()
    issue(0, 0)
    own_matrix.wait()
    for k in range(1, NY):
        y_copy(k).start()
    issue(1, 0)
    acc[...] = jnp.zeros_like(acc)
    lax.fori_loop(0, cols // 16, own_split, 0)
    for d in range(1, 4):
        with jax.named_scope(f"issue_0{d}"):
            issue(0, d)
        with jax.named_scope(f"issue_1{d}"):
            issue(1, d)
    with jax.named_scope("issue_20"):
        issue(2, 0)
    with jax.named_scope("issue_30"):
        issue(3, 0)
    with jax.named_scope("issue_21"):
        issue(2, 1)
    with jax.named_scope("y_wait"):
        for k in range(1, NY):
            y_wait(k)
            split_rows((y - k + NY) % NY)
    for m in (0, 1):
        for ahead in (True, False):
            ring_wait(m, 3, ahead)
    with jax.named_scope("multiply_0"):
        multiply(groups[0], 0, NZ)
    with jax.named_scope("spread_0"):
        pl.semaphore_wait(plane_sem, NY - 1)
        spread_partial(0)
    with jax.named_scope("issue_31"):
        issue(3, 1)
    with jax.named_scope("issue_22"):
        issue(2, 2)
    with jax.named_scope("issue_32"):
        issue(3, 2)
    multiply(late, 0, 3)
    with jax.named_scope("issue_23"):
        issue(2, 3)
    with jax.named_scope("issue_33"):
        issue(3, 3)
    multiply(late, 3, 4)
    multiply(late, 5, NZ)
    with jax.named_scope("total_0"):
        total_and_spread(0)
    for m in (2, 3):
        with jax.named_scope("last_wait"):
            for ahead in (True, False):
                ring_wait(m, 3, ahead)
        with jax.named_scope("multiply_last"):
            multiply(groups[m - 1], 4, 5)
        with jax.named_scope("spread_last"):
            spread_partial(m - 1)
    with jax.named_scope("total_1"):
        total_and_spread(1)
    with jax.named_scope("total_2"):
        total_and_spread(2)
    side = width // NY
    low = side // 2
    tile = 8
    s = y * NX + x
    partner = (x * 2 + 1 - core, c)
    rounds = (
        (6, piece_early, zland_early, packed_early),
        (4, piece_late, zland_late, packed_late),
    )

    def gram_part(turn):
        blocks, part_of, _, _ = rounds[turn]
        count = blocks // 2
        first = s * count // (low // tile)
        for n in range(2):
            b = (first + n) % blocks
            i, j = (b % 3, (b % 3 + b // 3) % 3) if turn == 0 else (b, 3)
            lh, ll = split(proj[:, lanes(i, side)].T)
            rh, rl = split(proj[:, lanes(j, side)])
            block[pl.ds(n * side, side), :] = product(lh, ll, rh, rl)
        for n in range(count):
            at = s * count + n
            row = (at // (low // tile) - first) * side + core * low + at % (low // tile) * tile
            part_of[pl.ds(n * tile, tile), :] = block[pl.ds(pl.multiple_of(row, tile), tile), :]

    def z_all(turn):
        _, part_of, landing, _ = rounds[turn]
        view = landing.at[pl.ds(0, (NZ - 1) * part_of.shape[0]), :]
        return pltpu.make_async_remote_copy(
            src_ref=view, dst_ref=view, send_sem=z_send.at[turn], recv_sem=z_recv.at[turn],
            device_id=z_peer(1), device_id_type=MESH,
        )

    def spread_z(turn):
        _, part_of, landing, _ = rounds[turn]
        own = lanes(z, part_of.shape[0])
        for k in Z_STEPS:
            pltpu.make_async_remote_copy(
                src_ref=part_of, dst_ref=landing.at[own, :],
                send_sem=z_send.at[turn], recv_sem=z_recv.at[turn],
                device_id=z_peer(k), device_id_type=MESH,
            ).start()
        landing[own, :] = part_of[...]

    def packed_rows(turn, of_core, of_y, of_x, chips):
        size = rounds[turn][1].shape[0]
        return pl.ds(pl.multiple_of(((of_core * NY + of_y) * NX + of_x) * size, size), chips * size)

    def spread_gram(turn):
        _, part_of, landing, packed = rounds[turn]
        size = part_of.shape[0]
        z_all(turn).wait_recv()
        total = landing[pl.ds(0, size), :]
        for k in range(1, NZ):
            total = total + landing[pl.ds(k * size, size), :]
        own = packed_rows(turn, core, y, x, 1)
        packed[own, :] = total
        for k in range(PLANE - 1):
            r2, _, c2 = plane_peer(k)
            if PEERS[k][2] == 0:
                pltpu.make_async_remote_copy(
                    src_ref=packed.at[own, :], dst_ref=packed.at[own, :],
                    send_sem=g_send.at[turn], recv_sem=g_recv.at[turn, PEERS[k][1]],
                    device_id=(r2, c2), device_id_type=MESH,
                ).start()

    def crossing(turn, of_core, ky):
        packed = rounds[turn][3]
        at = packed_rows(turn, of_core, (y - ky + NY) % NY, 0, NX)
        return pltpu.make_async_remote_copy(
            src_ref=packed.at[at, :], dst_ref=packed.at[at, :],
            send_sem=d_send.at[turn, ky], recv_sem=d_recv.at[turn, ky],
            device_id=partner, device_id_type=MESH,
        )

    def cross(turn):
        _, part_of, _, packed = rounds[turn]
        for ky in (0, 1, 3, 2):
            view = packed.at[pl.ds(0, (NX - 1 if ky == 0 else NX) * part_of.shape[0]), :]
            pltpu.make_async_remote_copy(
                src_ref=view, dst_ref=view, send_sem=g_send.at[turn], recv_sem=g_recv.at[turn, ky],
                device_id=partner, device_id_type=MESH,
            ).wait_recv()
            crossing(turn, core, ky).start()

    with jax.named_scope("proj_wait"):
        for group in range(2):
            all_of(proj, group, a_send, a_recv).wait_recv()
    gram_part(0)
    spread_z(0)
    with jax.named_scope("proj_wait_late"):
        all_of(proj, 2, a_send, a_recv).wait_recv()
    gram_part(1)
    spread_z(1)
    with jax.named_scope("z_wait"):
        spread_gram(0)
    with jax.named_scope("z_wait_late"):
        spread_gram(1)
    with jax.named_scope("cross"):
        cross(0)
    with jax.named_scope("cross_late"):
        cross(1)
    with jax.named_scope("partner_wait"):
        for turn in range(2):
            for ky in range(NY):
                crossing(turn, 1 - core, ky).wait_recv()
    own_cols[...] = proj[lanes(y, cols), :]

    with jax.named_scope("send_waits"):
        for copy in copies:
            copy.wait_send()
        for k in range(1, NY):
            y_copy(k).wait_send()
        for group in range(3):
            all_of(land, group, p_send, p_recv).wait_send()
            all_of(proj, group, a_send, a_recv).wait_send()
        for turn in range(2):
            _, part_of, _, packed = rounds[turn]
            z_all(turn).wait_send()
            view = packed.at[pl.ds(0, (NX * NY - 1) * part_of.shape[0]), :]
            pltpu.make_async_remote_copy(
                src_ref=view, dst_ref=view, send_sem=g_send.at[turn], recv_sem=g_recv.at[turn, 0],
                device_id=partner, device_id_type=MESH,
            ).wait_send()
            for ky in range(NY):
                crossing(turn, core, ky).wait_send()


def polar_kernel(packed_early, packed_late, own_cols, root, right, t, u_hi, u_lo, b_hi, b_lo, v):
    r, c = lax.axis_index("row"), lax.axis_index("col")
    width = t.shape[0]
    cols = own_cols.shape[0]
    wide_len, col_len = root.shape[1], root.shape[0]
    side = width // NY
    low = side // 2
    squares = jnp.zeros((low, side), F32)
    early = [(i, (i + o) % 3) for o in range(2) for i in range(3)]
    for packed, blocks in ((packed_early, early), (packed_late, [(i, 3) for i in range(4)])):
        for b, (i, j) in enumerate(blocks):
            for h in range(2):
                part_of = packed[pl.ds((h * len(blocks) + b) * low, low), :]
                squares = squares + (1.0 if i == j else 2.0) * (part_of * part_of)
                t[pl.ds(i * side + h * low, low), pl.ds(j * side, side)] = part_of
            if i != j:
                t[pl.ds(j * side, side), pl.ds(i * side, side)] = t[
                    pl.ds(i * side, side), pl.ds(j * side, side)
                ].T
    scale = jnp.sqrt(jnp.full((1, 1), jnp.sum(squares), F32) + 1e-06)
    root_scale = jnp.sqrt(scale)
    t[...] = t[...] * (1.0 / scale)

    size = width // 2
    a, b, full = pl.ds(0, size), pl.ds(size, size), pl.ds(0, width)
    tail = pl.ds(width, cols + col_len)
    b_tail = pl.ds(size, size + cols + col_len)
    v[pl.ds(0, cols), :] = own_cols[...]
    v[pl.ds(cols, col_len), :] = t[lanes(c, col_len), :]

    def put(slot, rows, at, value):
        hi, lo = split(value)
        u_hi[slot, rows, at] = hi
        u_lo[slot, rows, at] = lo

    def put_b(rows, at, value):
        hi, lo = split(value)
        b_hi[rows, at] = hi
        b_lo[rows, at] = lo

    def cut(value):
        return value[:size], value[size:]

    put(0, full, full, t[...])
    put(0, tail, full, v[...])
    for step in range(ITERS - 1):
        now, new = step % 2, (step + 1) % 2

        def by_t(rows, at):
            return product(
                u_hi[now, rows, :], u_lo[now, rows, :], u_hi[now, full, at], u_lo[now, full, at]
            )

        def by_b(rows, at):
            return product(u_hi[now, rows, :], u_lo[now, rows, :], b_hi[full, at], b_lo[full, at])

        if step == ITERS - 2:
            def times_t(value):
                hi, lo = split(value)
                both = jnp.concatenate([hi, lo], axis=0)
                dot = functools.partial(jnp.dot, preferred_element_type=F32)
                wide = dot(both, u_hi[now, full, :])
                rows = value.shape[0]
                return (wide[:rows] + wide[rows:]) + dot(hi, u_lo[now, full, :])

            def times_s(value):
                return 1.5 * value - 0.5 * times_t(value)

            value = times_s(v[...])
            v[...] = 1.5 * value - 0.5 * times_s(times_s(times_t(value)))
            break
        value = by_t(a, a)
        put_b(a, a, value)
        t[a, a] = 2.25 * t[a, a] - 1.5 * value
        value, left = cut(by_t(b_tail, a))
        put_b(b, a, value)
        put_b(a, b, value.T)
        t[b, a] = 2.25 * t[b, a] - 1.5 * value
        value, right_half = cut(by_t(b_tail, b))
        put_b(b, b, value)
        t[b, b] = 2.25 * t[b, b] - 1.5 * value
        first, second = cut(by_b(full, a))
        value = t[a, a] + 0.25 * first
        t[a, a] = value
        put(new, a, a, value)
        value = t[b, a] + 0.25 * second
        t[b, a] = value
        put(new, b, a, value)
        put(new, a, b, value.T)
        last = by_b(b, b)
        for at, moved in ((a, left), (b, right_half)):
            value = 1.5 * v[:, at] - 0.5 * moved
            v[:, at] = value
            put(new, tail, at, value)
        value = t[b, b] + 0.25 * last
        t[b, b] = value
        put(new, b, b, value)
    right[...] = v[pl.ds(0, cols), :] * (1.0 / root_scale)
    ours = v[pl.ds(cols, col_len), :] * root_scale
    turn = (width - r * wide_len) % width
    root[...] = pltpu.roll(ours, turn, 1)[:, :wide_len]


def local(matrix, basis):
    cols, depth = matrix.shape
    rows, width = basis.shape
    part = depth // NY
    side = width // NY
    early, late = 6 * side // (2 * NX * NY), 4 * side // (2 * NX * NY)
    row_len, col_len = width // NR, width // (NY * NZ)
    dma = pltpu.SemaphoreType.DMA
    vmem = pl.BlockSpec(memory_space=pltpu.VMEM)
    hbm = pl.BlockSpec(memory_space=pltpu.HBM)
    packed_early, packed_late, own_cols = pl.pallas_call(
        gather_kernel,
        name="gather",
        out_shape=(
            jax.ShapeDtypeStruct((PLANE * early, side), F32),
            jax.ShapeDtypeStruct((PLANE * late, side), F32),
            jax.ShapeDtypeStruct((cols, width), F32),
        ),
        in_specs=[hbm, hbm],
        out_specs=(vmem, vmem, vmem),
        scratch_shapes=[
            pltpu.VMEM((cols, depth), F32),
            pltpu.VMEM((NY * cols, part), F32),
            pltpu.VMEM((NY * cols, part), BF16),
            pltpu.VMEM((NY * cols, part), BF16),
            pltpu.VMEM((NZ * rows, width), F32),
            pltpu.VMEM((NY * cols, width), F32),
            pltpu.VMEM(((PLANE - 1) * cols // NR, width), F32),
            pltpu.VMEM((NY * cols, width), F32),
            pltpu.VMEM((2 * side, side), F32),
            pltpu.VMEM((early, side), F32),
            pltpu.VMEM((late, side), F32),
            pltpu.VMEM((NZ * early, side), F32),
            pltpu.VMEM((NZ * late, side), F32),
            dma((NY - 1,)), dma((NY - 1,)),
            dma((4, 4)), dma((4, 4)), dma((4, 4)), dma((4, 4)), dma((2,)),
            dma((3,)), dma((3,)), dma((3,)), dma((3,)),
            dma((2,)), dma((2,)), dma((2,)), dma((2, NY)), dma((2, NY)), dma((2, NY)),
            pltpu.SemaphoreType.REGULAR,
        ],
        compiler_params=pltpu.CompilerParams(
            collective_id=0, has_side_effects=True, vmem_limit_bytes=48 * 2**20
        ),
    )(*(pltpu.with_memory_space_constraint(a, pltpu.HBM) for a in (matrix, basis)))
    root, right = pl.pallas_call(
        polar_kernel,
        name="polar",
        out_shape=(
            jax.ShapeDtypeStruct((col_len, row_len), F32),
            jax.ShapeDtypeStruct((cols, width), F32),
        ),
        in_specs=[vmem, vmem, vmem],
        out_specs=(vmem, vmem),
        scratch_shapes=[
            pltpu.VMEM((width, width), F32),
            pltpu.VMEM((2, width + cols + col_len, width), BF16),
            pltpu.VMEM((2, width + cols + col_len, width), BF16),
            pltpu.VMEM((width, width), BF16),
            pltpu.VMEM((width, width), BF16),
            pltpu.VMEM((cols + col_len, width), F32),
        ],
        compiler_params=pltpu.CompilerParams(vmem_limit_bytes=24 * 2**20),
    )(packed_early, packed_late, own_cols)
    return root.T, right


def solution(mesh):
    return jax.shard_map(
        local,
        mesh=mesh,
        in_specs=(P("col", "row"), P(("row", "col"), None)),
        out_specs=(P("row", "col"), P("col", None)),
        check_vma=False,
    )
```

```python
import functools

import jax
import jax.numpy as jnp
from jax import lax
from jax.experimental import pallas as pl
from jax.experimental.pallas import tpu as pltpu
from jax.sharding import PartitionSpec as P

MESH = pl.DeviceIdType.MESH
ITERS = 8
F32 = jnp.float32
BF16 = jnp.bfloat16
NX, NY, NZ = 4, 4, 8
NR, PLANE = 2 * NX, 2 * NX * NY


def split(a):
    hi = a.astype(BF16)
    return hi, (a - hi.astype(F32)).astype(BF16)


def product(ah, al, bh, bl, dims=(((1,), (0,)), ((), ()))):
    dot = functools.partial(
        lax.dot_general, dimension_numbers=dims, preferred_element_type=F32
    )
    return dot(ah, bh) + (dot(ah, bl) + dot(al, bh))


PEERS = sorted(
    [(dx, dy, dc) for dx in range(NX) for dy in range(NY) for dc in range(2)][1:],
    key=lambda p: -(min(p[0], NX - p[0]) * 2 + min(p[1], NY - p[1]) * 2 + p[2]),
)
Z_STEPS = sorted(range(1, NZ), key=lambda d: -min(d, NZ - d))


def lanes(i, size):
    return pl.ds(pl.multiple_of(i * size, size), size)


def gather_kernel(
    mat_hbm, bas_hbm, packed_early, packed_late, own_cols,
    mat, m_in, m_hi, m_lo, q, acc, land, proj, block,
    piece_early, piece_late, zland_early, zland_late,
    y_send, y_recv, f_send, f_recv, b_send, b_recv, local_sem,
    p_send, p_recv, a_send, a_recv, z_send, z_recv, g_send, g_recv, d_send, d_recv, plane_sem,
):
    r, c = lax.axis_index("row"), lax.axis_index("col")
    y, z = c // NZ, c % NZ
    x, core = r // 2, r % 2
    cols = mat.shape[0]
    part = mat.shape[1] // NY
    rows, width = bas_hbm.shape
    half = rows // 2
    wide = width // 4
    piece = cols // NR

    near_x = [(x + d) % NX for d in range(NX)]
    near_y = [(y + d) % NY for d in range(NY)]
    near_row = [[n * 2 + (core + d) % 2 for d in range(2)] for n in near_x]
    near_col = [n * NZ + z for n in near_y]

    def plane_peer(k):
        dx, dy, dc = PEERS[k]
        return near_row[dx][dc], near_y[dy], near_col[dy]

    def z_peer(k):
        return (r, y * NZ + (z + k) % NZ)

    own_basis = pltpu.make_async_copy(bas_hbm, q.at[lanes(z, rows), :], local_sem.at[0])
    own_basis.start()
    own_matrix = pltpu.make_async_copy(mat_hbm, mat, local_sem.at[1])
    own_matrix.start()

    barrier = pltpu.get_barrier_semaphore()

    near = [z_peer(1), z_peer(NZ - 1)] + [(r, near_col[d]) for d in range(1, NY)]
    for k in range(PLANE - 1):
        if PEERS[k][1] == 0:
            near.append((plane_peer(k)[0], c))
    for peer in near:
        pl.semaphore_signal(barrier, inc=1, device_id=peer, device_id_type=MESH)
    with jax.named_scope("barrier"):
        pl.semaphore_wait(barrier, len(near))
    for d in range(1, NY):
        pl.semaphore_signal(plane_sem, inc=1, device_id=(r, near_col[d]), device_id_type=MESH)

    def ring_item(m, d, part, ahead, behind):
        owner = (z - (behind if ahead else -behind) + NZ) % NZ
        span = pl.ds(pl.multiple_of(owner * rows, rows), rows)
        if part is not None:
            start = owner * rows + (0 if ahead == (part == 0) else half)
            span = pl.ds(pl.multiple_of(start, half), half)
        view = q.at[span, pl.ds(m * wide, wide)]
        send, recv = (f_send, f_recv) if ahead else (b_send, b_recv)
        at = d + 3 * (part or 0)
        return pltpu.make_async_remote_copy(
            src_ref=view, dst_ref=view, send_sem=send.at[m, at], recv_sem=recv.at[m, at],
            device_id=(r, y * NZ + (z + (1 if ahead else -1) + NZ) % NZ), device_id_type=MESH,
        )

    def ring_wait(m, d, part=None):
        for ahead in (True, False):
            ring_item(m, d, part, ahead, d + 1).wait_recv()

    def y_copy(k):
        y2 = (y + k) % NY
        return pltpu.make_async_remote_copy(
            src_ref=mat.at[:, lanes(y2, part)], dst_ref=m_in.at[lanes(y, cols), :],
            send_sem=y_send.at[k - 1], recv_sem=y_recv.at[k - 1],
            device_id=(r, y2 * NZ + z), device_id_type=MESH,
        )

    def y_wait(k):
        src = (y - k + NY) % NY
        pltpu.make_async_remote_copy(
            src_ref=mat.at[:, lanes(src, part)], dst_ref=m_in.at[lanes(src, cols), :],
            send_sem=y_send.at[k - 1], recv_sem=y_recv.at[k - 1],
            device_id=(r, src * NZ + z), device_id_type=MESH,
        ).wait_recv()

    copies = []

    def issue(m, d, part=None):
        for ahead in (True, False):
            copy = ring_item(m, d, part, ahead, d)
            copy.start()
            copies.append(copy)

    def split_rows(src):
        def one(i, _):
            at = pl.ds(pl.multiple_of(i * 16, 16), 16)
            hi, lo = split(m_in[at, :])
            m_hi[at, :] = hi
            m_lo[at, :] = lo
            return 0

        lax.fori_loop(src * (cols // 16), (src + 1) * (cols // 16), one, 0)

    def own_split(i, _):
        hi, lo = split(mat[pl.ds(pl.multiple_of(i * 16, 16), 16), lanes(y, part)])
        at = pl.ds(pl.multiple_of(y * cols + i * 16, 16), 16)
        m_hi[at, :] = hi
        m_lo[at, :] = lo
        return 0

    groups = [pl.ds(0, 2 * wide), pl.ds(2 * wide, wide), pl.ds(3 * wide, wide)]

    def multiply(here, first, last):

        def one(o, _):
            owner = (z + o) % NZ
            qh, ql = split(q[lanes(owner, rows), here])
            at = lanes(owner, rows)
            acc[:, here] += product(m_hi[:, at], m_lo[:, at], qh, ql)
            return 0

        lax.fori_loop(first, last, one, 0)

    def spread_partial(group):
        here = groups[group]

        for k in range(PLANE - 1):
            r2, y2, c2 = plane_peer(k)
            src = pl.ds(pl.multiple_of(y2 * cols + r2 * piece, piece), piece)
            pltpu.make_async_remote_copy(
                src_ref=acc.at[src, here], dst_ref=land.at[pl.ds(k * piece, piece), here],
                send_sem=p_send.at[group], recv_sem=p_recv.at[group],
                device_id=(r2, c2), device_id_type=MESH,
            ).start()

    mine = pl.ds(pl.multiple_of(y * cols + r * piece, piece), piece)

    def all_of(ref, group, send, recv):
        view = ref.at[pl.ds(0, (PLANE - 1) * piece), groups[group]]
        return pltpu.make_async_remote_copy(
            src_ref=view, dst_ref=view, send_sem=send.at[group], recv_sem=recv.at[group],
            device_id=z_peer(1), device_id_type=MESH,
        )

    def total_and_spread(group):
        here = groups[group]
        all_of(land, group, p_send, p_recv).wait_recv()
        total = acc[mine, here]
        for k in range(PLANE - 1):
            total = total + land[pl.ds(k * piece, piece), here]
        proj[mine, here] = total

        for k in range(PLANE - 1):
            r2, _, c2 = plane_peer(k)
            pltpu.make_async_remote_copy(
                src_ref=proj.at[mine, here], dst_ref=proj.at[mine, here],
                send_sem=a_send.at[group], recv_sem=a_recv.at[group],
                device_id=(r2, c2), device_id_type=MESH,
            ).start()

    own_basis.wait()
    issue(0, 0)
    own_matrix.wait()
    for k in range(1, NY):
        y_copy(k).start()
    issue(1, 0)
    acc[...] = jnp.zeros_like(acc)
    lax.fori_loop(0, cols // 16, own_split, 0)
    for m, d in ((0, 1), (1, 1), (0, 2), (1, 2)):
        with jax.named_scope(f"issue_{m}{d}"):
            ring_wait(m, d - 1)
            issue(m, d)
    issue(2, 0)
    issue(3, 0)
    with jax.named_scope("issue_21"):
        for m in (0, 1):
            ring_wait(m, 2)
        ring_wait(2, 0)
        issue(2, 1)
    issue(0, 3, 0)
    issue(1, 3, 0)
    with jax.named_scope("issue_31"):
        ring_wait(3, 0)
    with jax.named_scope("issue_22"):
        ring_wait(2, 1)
        issue(2, 2)
    for which in (0, 1):
        issue(3, 1, which)
    with jax.named_scope("y_wait"):
        for k in range(1, NY):
            y_wait(k)
            split_rows((y - k + NY) % NY)
    with jax.named_scope("wait_03"):
        for m in (0, 1):
            ring_wait(m, 3, 0)
    with jax.named_scope("multiply_0"):
        multiply(groups[0], 0, NZ)
    with jax.named_scope("spread_0"):
        pl.semaphore_wait(plane_sem, NY - 1)
        spread_partial(0)
    with jax.named_scope("multiply_1a"):
        ring_wait(2, 2)
        multiply(groups[1], 0, 4)
    with jax.named_scope("issue_320"):
        ring_wait(3, 1, 0)
        issue(3, 2, 0)
        issue(2, 3, 0)
    with jax.named_scope("multiply_1b"):
        multiply(groups[1], 5, NZ)
    with jax.named_scope("issue_321"):
        ring_wait(3, 1, 1)
        issue(3, 2, 1)
    with jax.named_scope("multiply_2"):
        multiply(groups[2], 0, 3)
        multiply(groups[2], 6, NZ)
    with jax.named_scope("issue_33"):
        ring_wait(3, 2, 0)
        issue(3, 3, 0)
    with jax.named_scope("wait_23"):
        ring_wait(2, 3, 0)
    with jax.named_scope("spread_1"):
        multiply(groups[1], 4, 5)
        spread_partial(1)
    with jax.named_scope("wait_32"):
        ring_wait(3, 2, 1)
        multiply(groups[2], 3, 4)
        multiply(groups[2], 5, 6)
    with jax.named_scope("total_0"):
        total_and_spread(0)
    with jax.named_scope("last_wait"):
        ring_wait(3, 3, 0)
    with jax.named_scope("spread_2"):
        multiply(groups[2], 4, 5)
        spread_partial(2)
    with jax.named_scope("total_1"):
        total_and_spread(1)
    with jax.named_scope("total_2"):
        total_and_spread(2)

    side = width // NY
    low = side // 2
    tile = 8
    s = y * NX + x
    partner = (x * 2 + 1 - core, c)
    rounds = (
        (6, piece_early, zland_early, packed_early),
        (4, piece_late, zland_late, packed_late),
    )

    def gram_part(turn):
        blocks, part_of, _, _ = rounds[turn]
        count = blocks // 2
        first = s * count // (low // tile)
        for n in range(2):
            b = (first + n) % blocks
            i, j = (b % 3, (b % 3 + b // 3) % 3) if turn == 0 else (b, 3)
            lh, ll = split(proj[:, lanes(i, side)].T)
            rh, rl = split(proj[:, lanes(j, side)])
            block[pl.ds(n * side, side), :] = product(lh, ll, rh, rl)
        for n in range(count):
            at = s * count + n
            row = (at // (low // tile) - first) * side + core * low + at % (low // tile) * tile
            part_of[pl.ds(n * tile, tile), :] = block[pl.ds(pl.multiple_of(row, tile), tile), :]

    def z_all(turn):
        _, part_of, landing, _ = rounds[turn]
        view = landing.at[pl.ds(0, (NZ - 1) * part_of.shape[0]), :]
        return pltpu.make_async_remote_copy(
            src_ref=view, dst_ref=view, send_sem=z_send.at[turn], recv_sem=z_recv.at[turn],
            device_id=z_peer(1), device_id_type=MESH,
        )

    def spread_z(turn):
        _, part_of, landing, _ = rounds[turn]
        own = lanes(z, part_of.shape[0])
        for k in Z_STEPS:
            pltpu.make_async_remote_copy(
                src_ref=part_of, dst_ref=landing.at[own, :],
                send_sem=z_send.at[turn], recv_sem=z_recv.at[turn],
                device_id=z_peer(k), device_id_type=MESH,
            ).start()
        landing[own, :] = part_of[...]

    def packed_rows(turn, of_core, of_y, of_x, chips):
        size = rounds[turn][1].shape[0]
        return pl.ds(pl.multiple_of(((of_core * NY + of_y) * NX + of_x) * size, size), chips * size)

    def spread_gram(turn):
        _, part_of, landing, packed = rounds[turn]
        size = part_of.shape[0]
        z_all(turn).wait_recv()
        total = landing[pl.ds(0, size), :]
        for k in range(1, NZ):
            total = total + landing[pl.ds(k * size, size), :]
        own = packed_rows(turn, core, y, x, 1)
        packed[own, :] = total
        for k in range(PLANE - 1):
            r2, _, c2 = plane_peer(k)
            if PEERS[k][2] == 0:
                pltpu.make_async_remote_copy(
                    src_ref=packed.at[own, :], dst_ref=packed.at[own, :],
                    send_sem=g_send.at[turn], recv_sem=g_recv.at[turn, PEERS[k][1]],
                    device_id=(r2, c2), device_id_type=MESH,
                ).start()

    def crossing(turn, of_core, ky):
        packed = rounds[turn][3]
        at = packed_rows(turn, of_core, (y - ky + NY) % NY, 0, NX)
        return pltpu.make_async_remote_copy(
            src_ref=packed.at[at, :], dst_ref=packed.at[at, :],
            send_sem=d_send.at[turn, ky], recv_sem=d_recv.at[turn, ky],
            device_id=partner, device_id_type=MESH,
        )

    def cross(turn):
        _, part_of, _, packed = rounds[turn]
        for ky in (0, 1, 3, 2):
            view = packed.at[pl.ds(0, (NX - 1 if ky == 0 else NX) * part_of.shape[0]), :]
            pltpu.make_async_remote_copy(
                src_ref=view, dst_ref=view, send_sem=g_send.at[turn], recv_sem=g_recv.at[turn, ky],
                device_id=partner, device_id_type=MESH,
            ).wait_recv()
            crossing(turn, core, ky).start()

    with jax.named_scope("proj_wait"):
        for group in range(2):
            all_of(proj, group, a_send, a_recv).wait_recv()
    gram_part(0)
    spread_z(0)
    with jax.named_scope("proj_wait_late"):
        all_of(proj, 2, a_send, a_recv).wait_recv()
    gram_part(1)
    spread_z(1)
    with jax.named_scope("z_wait"):
        spread_gram(0)
    with jax.named_scope("z_wait_late"):
        spread_gram(1)
    with jax.named_scope("cross"):
        cross(0)
    with jax.named_scope("cross_late"):
        cross(1)
    with jax.named_scope("partner_wait"):
        for turn in range(2):
            for ky in range(NY):
                crossing(turn, 1 - core, ky).wait_recv()
    own_cols[...] = proj[lanes(y, cols), :]

    with jax.named_scope("send_waits"):
        for copy in copies:
            copy.wait_send()
        for k in range(1, NY):
            y_copy(k).wait_send()
        for group in range(3):
            all_of(land, group, p_send, p_recv).wait_send()
            all_of(proj, group, a_send, a_recv).wait_send()
        for turn in range(2):
            _, part_of, _, packed = rounds[turn]
            z_all(turn).wait_send()
            view = packed.at[pl.ds(0, (NX * NY - 1) * part_of.shape[0]), :]
            pltpu.make_async_remote_copy(
                src_ref=view, dst_ref=view, send_sem=g_send.at[turn], recv_sem=g_recv.at[turn, 0],
                device_id=partner, device_id_type=MESH,
            ).wait_send()
            for ky in range(NY):
                crossing(turn, core, ky).wait_send()


def polar_kernel(packed_early, packed_late, own_cols, root, right, t, u_hi, u_lo, b_hi, b_lo, v):
    r, c = lax.axis_index("row"), lax.axis_index("col")
    width = t.shape[0]
    cols = own_cols.shape[0]
    wide_len, col_len = root.shape[1], root.shape[0]
    side = width // NY
    low = side // 2
    squares = jnp.zeros((low, side), F32)
    early = [(i, (i + o) % 3) for o in range(2) for i in range(3)]
    for packed, blocks in ((packed_early, early), (packed_late, [(i, 3) for i in range(4)])):
        for b, (i, j) in enumerate(blocks):
            for h in range(2):
                part_of = packed[pl.ds((h * len(blocks) + b) * low, low), :]
                squares = squares + (1.0 if i == j else 2.0) * (part_of * part_of)
                t[pl.ds(i * side + h * low, low), pl.ds(j * side, side)] = part_of
            if i != j:
                t[pl.ds(j * side, side), pl.ds(i * side, side)] = t[
                    pl.ds(i * side, side), pl.ds(j * side, side)
                ].T
    scale = jnp.sqrt(jnp.full((1, 1), jnp.sum(squares), F32) + 1e-06)
    root_scale = jnp.sqrt(scale)
    t[...] = t[...] * (1.0 / scale)

    size = width // 2
    a, b, full = pl.ds(0, size), pl.ds(size, size), pl.ds(0, width)
    tail = pl.ds(width, cols + col_len)
    b_tail = pl.ds(size, size + cols + col_len)
    v[pl.ds(0, cols), :] = own_cols[...]
    v[pl.ds(cols, col_len), :] = t[lanes(c, col_len), :]

    def put(slot, rows, at, value):
        hi, lo = split(value)
        u_hi[slot, rows, at] = hi
        u_lo[slot, rows, at] = lo

    def put_b(rows, at, value):
        hi, lo = split(value)
        b_hi[rows, at] = hi
        b_lo[rows, at] = lo

    def cut(value):
        return value[:size], value[size:]

    put(0, full, full, t[...])
    put(0, tail, full, v[...])
    for step in range(ITERS - 1):
        now, new = step % 2, (step + 1) % 2

        def by_t(rows, at):
            return product(
                u_hi[now, rows, :], u_lo[now, rows, :], u_hi[now, full, at], u_lo[now, full, at]
            )

        def by_b(rows, at):
            return product(u_hi[now, rows, :], u_lo[now, rows, :], b_hi[full, at], b_lo[full, at])

        if step == ITERS - 2:
            def times_t(value):
                hi, lo = split(value)
                both = jnp.concatenate([hi, lo], axis=0)
                dot = functools.partial(jnp.dot, preferred_element_type=F32)
                wide = dot(both, u_hi[now, full, :])
                rows = value.shape[0]
                return (wide[:rows] + wide[rows:]) + dot(hi, u_lo[now, full, :])

            def times_s(value):
                return 1.5 * value - 0.5 * times_t(value)

            value = times_s(v[...])
            v[...] = 1.5 * value - 0.5 * times_s(times_s(times_t(value)))
            break
        value = by_t(a, a)
        put_b(a, a, value)
        t[a, a] = 2.25 * t[a, a] - 1.5 * value
        value, left = cut(by_t(b_tail, a))
        put_b(b, a, value)
        put_b(a, b, value.T)
        t[b, a] = 2.25 * t[b, a] - 1.5 * value
        value, right_half = cut(by_t(b_tail, b))
        put_b(b, b, value)
        t[b, b] = 2.25 * t[b, b] - 1.5 * value
        first, second = cut(by_b(full, a))
        value = t[a, a] + 0.25 * first
        t[a, a] = value
        put(new, a, a, value)
        value = t[b, a] + 0.25 * second
        t[b, a] = value
        put(new, b, a, value)
        put(new, a, b, value.T)
        last = by_b(b, b)
        for at, moved in ((a, left), (b, right_half)):
            value = 1.5 * v[:, at] - 0.5 * moved
            v[:, at] = value
            put(new, tail, at, value)
        value = t[b, b] + 0.25 * last
        t[b, b] = value
        put(new, b, b, value)
    right[...] = v[pl.ds(0, cols), :] * (1.0 / root_scale)
    ours = v[pl.ds(cols, col_len), :] * root_scale
    turn = (width - r * wide_len) % width
    root[...] = pltpu.roll(ours, turn, 1)[:, :wide_len]


def local(matrix, basis):
    cols, depth = matrix.shape
    rows, width = basis.shape
    part = depth // NY
    side = width // NY
    early, late = 6 * side // (2 * NX * NY), 4 * side // (2 * NX * NY)
    row_len, col_len = width // NR, width // (NY * NZ)
    dma = pltpu.SemaphoreType.DMA
    vmem = pl.BlockSpec(memory_space=pltpu.VMEM)
    hbm = pl.BlockSpec(memory_space=pltpu.HBM)
    packed_early, packed_late, own_cols = pl.pallas_call(
        gather_kernel,
        name="gather",
        out_shape=(
            jax.ShapeDtypeStruct((PLANE * early, side), F32),
            jax.ShapeDtypeStruct((PLANE * late, side), F32),
            jax.ShapeDtypeStruct((cols, width), F32),
        ),
        in_specs=[hbm, hbm],
        out_specs=(vmem, vmem, vmem),
        scratch_shapes=[
            pltpu.VMEM((cols, depth), F32),
            pltpu.VMEM((NY * cols, part), F32),
            pltpu.VMEM((NY * cols, part), BF16),
            pltpu.VMEM((NY * cols, part), BF16),
            pltpu.VMEM((NZ * rows, width), F32),
            pltpu.VMEM((NY * cols, width), F32),
            pltpu.VMEM(((PLANE - 1) * cols // NR, width), F32),
            pltpu.VMEM((NY * cols, width), F32),
            pltpu.VMEM((2 * side, side), F32),
            pltpu.VMEM((early, side), F32),
            pltpu.VMEM((late, side), F32),
            pltpu.VMEM((NZ * early, side), F32),
            pltpu.VMEM((NZ * late, side), F32),
            dma((NY - 1,)), dma((NY - 1,)),
            dma((4, 6)), dma((4, 6)), dma((4, 6)), dma((4, 6)), dma((2,)),
            dma((3,)), dma((3,)), dma((3,)), dma((3,)),
            dma((2,)), dma((2,)), dma((2,)), dma((2, NY)), dma((2, NY)), dma((2, NY)),
            pltpu.SemaphoreType.REGULAR,
        ],
        compiler_params=pltpu.CompilerParams(
            collective_id=0, has_side_effects=True, vmem_limit_bytes=48 * 2**20
        ),
    )(*(pltpu.with_memory_space_constraint(a, pltpu.HBM) for a in (matrix, basis)))
    root, right = pl.pallas_call(
        polar_kernel,
        name="polar",
        out_shape=(
            jax.ShapeDtypeStruct((col_len, row_len), F32),
            jax.ShapeDtypeStruct((cols, width), F32),
        ),
        in_specs=[vmem, vmem, vmem],
        out_specs=(vmem, vmem),
        scratch_shapes=[
            pltpu.VMEM((width, width), F32),
            pltpu.VMEM((2, width + cols + col_len, width), BF16),
            pltpu.VMEM((2, width + cols + col_len, width), BF16),
            pltpu.VMEM((width, width), BF16),
            pltpu.VMEM((width, width), BF16),
            pltpu.VMEM((cols + col_len, width), F32),
        ],
        compiler_params=pltpu.CompilerParams(vmem_limit_bytes=24 * 2**20),
    )(packed_early, packed_late, own_cols)
    return root.T, right


def solution(mesh):
    return jax.shard_map(
        local,
        mesh=mesh,
        in_specs=(P("col", "row"), P(("row", "col"), None)),
        out_specs=(P("row", "col"), P("col", None)),
        check_vma=False,
    )
```

```python
import functools

import jax
import jax.numpy as jnp
from jax import lax
from jax.experimental import pallas as pl
from jax.experimental.pallas import tpu as pltpu
from jax.sharding import PartitionSpec as P

MESH = pl.DeviceIdType.MESH
ITERS = 8
F32 = jnp.float32
BF16 = jnp.bfloat16
NX, NY, NZ = 4, 4, 8
NR, PLANE = 2 * NX, 2 * NX * NY


def split(a):
    hi = a.astype(BF16)
    return hi, (a - hi.astype(F32)).astype(BF16)


def product(ah, al, bh, bl, dims=(((1,), (0,)), ((), ()))):
    dot = functools.partial(
        lax.dot_general, dimension_numbers=dims, preferred_element_type=F32
    )
    return dot(ah, bh) + (dot(ah, bl) + dot(al, bh))


PEERS = sorted(
    [(dx, dy, dc) for dx in range(NX) for dy in range(NY) for dc in range(2)][1:],
    key=lambda p: -(min(p[0], NX - p[0]) * 2 + min(p[1], NY - p[1]) * 2 + p[2]),
)
Z_STEPS = sorted(range(1, NZ), key=lambda d: -min(d, NZ - d))


def lanes(i, size):
    return pl.ds(pl.multiple_of(i * size, size), size)


def gather_kernel(
    mat_hbm, bas_hbm, packed_early, packed_late, own_cols,
    mat, m_in, m_hi, m_lo, q, acc, land, proj, block,
    piece_early, piece_late, zland_early, zland_late,
    y_send, y_recv, f_send, f_recv, b_send, b_recv, local_sem,
    p_send, p_recv, a_send, a_recv, z_send, z_recv, g_send, g_recv, d_send, d_recv, plane_sem,
):
    r, c = lax.axis_index("row"), lax.axis_index("col")
    y, z = c // NZ, c % NZ
    x, core = r // 2, r % 2
    cols = mat.shape[0]
    part = mat.shape[1] // NY
    rows, width = bas_hbm.shape
    half = rows // 2
    wide = width // 4
    piece = cols // NR

    near_x = [(x + d) % NX for d in range(NX)]
    near_y = [(y + d) % NY for d in range(NY)]
    near_row = [[n * 2 + (core + d) % 2 for d in range(2)] for n in near_x]
    near_col = [n * NZ + z for n in near_y]

    def plane_peer(k):
        dx, dy, dc = PEERS[k]
        return near_row[dx][dc], near_y[dy], near_col[dy]

    def z_peer(k):
        return (r, y * NZ + (z + k) % NZ)

    own_basis = pltpu.make_async_copy(bas_hbm, q.at[lanes(z, rows), :], local_sem.at[0])
    own_basis.start()
    own_matrix = pltpu.make_async_copy(mat_hbm, mat, local_sem.at[1])
    own_matrix.start()

    barrier = pltpu.get_barrier_semaphore()

    near = [z_peer(1), z_peer(NZ - 1)] + [(r, near_col[d]) for d in range(1, NY)]
    for k in range(PLANE - 1):
        if PEERS[k][1] == 0:
            near.append((plane_peer(k)[0], c))
    for peer in near:
        pl.semaphore_signal(barrier, inc=1, device_id=peer, device_id_type=MESH)
    with jax.named_scope("barrier"):
        pl.semaphore_wait(barrier, len(near))
    for d in range(1, NY):
        pl.semaphore_signal(plane_sem, inc=1, device_id=(r, near_col[d]), device_id_type=MESH)

    def ring_item(m, d, part, ahead, behind):
        owner = (z - (behind if ahead else -behind) + NZ) % NZ
        span = pl.ds(pl.multiple_of(owner * rows, rows), rows)
        if part is not None:
            start = owner * rows + (0 if ahead == (part == 0) else half)
            span = pl.ds(pl.multiple_of(start, half), half)
        view = q.at[span, pl.ds(m * wide, wide)]
        send, recv = (f_send, f_recv) if ahead else (b_send, b_recv)
        at = d + 3 * (part or 0)
        return pltpu.make_async_remote_copy(
            src_ref=view, dst_ref=view, send_sem=send.at[m, at], recv_sem=recv.at[m, at],
            device_id=(r, y * NZ + (z + (1 if ahead else -1) + NZ) % NZ), device_id_type=MESH,
        )

    def ring_wait(m, d, part=None):
        for ahead in (True, False):
            ring_item(m, d, part, ahead, d + 1).wait_recv()

    def y_copy(k):
        y2 = (y + k) % NY
        return pltpu.make_async_remote_copy(
            src_ref=mat.at[:, lanes(y2, part)], dst_ref=m_in.at[lanes(y, cols), :],
            send_sem=y_send.at[k - 1], recv_sem=y_recv.at[k - 1],
            device_id=(r, y2 * NZ + z), device_id_type=MESH,
        )

    def y_wait(k):
        src = (y - k + NY) % NY
        pltpu.make_async_remote_copy(
            src_ref=mat.at[:, lanes(src, part)], dst_ref=m_in.at[lanes(src, cols), :],
            send_sem=y_send.at[k - 1], recv_sem=y_recv.at[k - 1],
            device_id=(r, src * NZ + z), device_id_type=MESH,
        ).wait_recv()

    copies = []

    def issue(m, d, part=None):
        for ahead in (True, False):
            copy = ring_item(m, d, part, ahead, d)
            copy.start()
            copies.append(copy)

    def split_rows(src):
        def one(i, _):
            at = pl.ds(pl.multiple_of(i * 16, 16), 16)
            hi, lo = split(m_in[at, :])
            m_hi[at, :] = hi
            m_lo[at, :] = lo
            return 0

        lax.fori_loop(src * (cols // 16), (src + 1) * (cols // 16), one, 0)

    def own_split(i, _):
        hi, lo = split(mat[pl.ds(pl.multiple_of(i * 16, 16), 16), lanes(y, part)])
        at = pl.ds(pl.multiple_of(y * cols + i * 16, 16), 16)
        m_hi[at, :] = hi
        m_lo[at, :] = lo
        return 0

    groups = [pl.ds(0, 2 * wide), pl.ds(2 * wide, wide), pl.ds(3 * wide, wide)]

    def multiply(here, first, last):

        def one(o, _):
            owner = (z + o) % NZ
            qh, ql = split(q[lanes(owner, rows), here])
            at = lanes(owner, rows)
            acc[:, here] += product(m_hi[:, at], m_lo[:, at], qh, ql)
            return 0

        lax.fori_loop(first, last, one, 0)

    def spread_partial(group):
        here = groups[group]

        for k in range(PLANE - 1):
            r2, y2, c2 = plane_peer(k)
            src = pl.ds(pl.multiple_of(y2 * cols + r2 * piece, piece), piece)
            pltpu.make_async_remote_copy(
                src_ref=acc.at[src, here], dst_ref=land.at[pl.ds(k * piece, piece), here],
                send_sem=p_send.at[group], recv_sem=p_recv.at[group],
                device_id=(r2, c2), device_id_type=MESH,
            ).start()

    mine = pl.ds(pl.multiple_of(y * cols + r * piece, piece), piece)

    def all_of(ref, group, send, recv):
        view = ref.at[pl.ds(0, (PLANE - 1) * piece), groups[group]]
        return pltpu.make_async_remote_copy(
            src_ref=view, dst_ref=view, send_sem=send.at[group], recv_sem=recv.at[group],
            device_id=z_peer(1), device_id_type=MESH,
        )

    def total_and_spread(group):
        here = groups[group]
        all_of(land, group, p_send, p_recv).wait_recv()
        total = acc[mine, here]
        for k in range(PLANE - 1):
            total = total + land[pl.ds(k * piece, piece), here]
        proj[mine, here] = total

        for k in range(PLANE - 1):
            r2, _, c2 = plane_peer(k)
            pltpu.make_async_remote_copy(
                src_ref=proj.at[mine, here], dst_ref=proj.at[mine, here],
                send_sem=a_send.at[group], recv_sem=a_recv.at[group],
                device_id=(r2, c2), device_id_type=MESH,
            ).start()

    own_basis.wait()
    issue(0, 0)
    own_matrix.wait()
    for k in range(1, NY):
        y_copy(k).start()
    issue(1, 0)
    acc[...] = jnp.zeros_like(acc)
    lax.fori_loop(0, cols // 16, own_split, 0)
    for m, d in ((0, 1), (1, 1), (0, 2), (1, 2)):
        with jax.named_scope(f"issue_{m}{d}"):
            ring_wait(m, d - 1)
            issue(m, d)
    issue(2, 0)
    issue(3, 0)
    with jax.named_scope("issue_21"):
        for m in (0, 1):
            ring_wait(m, 2)
        ring_wait(2, 0)
        issue(2, 1)
    issue(0, 3, 0)
    issue(1, 3, 0)
    with jax.named_scope("issue_31"):
        ring_wait(3, 0)
    with jax.named_scope("issue_22"):
        ring_wait(2, 1)
        issue(2, 2)
    for which in (0, 1):
        issue(3, 1, which)
    with jax.named_scope("y_wait"):
        for k in range(1, NY):
            y_wait(k)
            split_rows((y - k + NY) % NY)
    with jax.named_scope("wait_03"):
        for m in (0, 1):
            ring_wait(m, 3, 0)
    with jax.named_scope("multiply_0"):
        multiply(groups[0], 0, NZ)
    with jax.named_scope("spread_0"):
        pl.semaphore_wait(plane_sem, NY - 1)
        spread_partial(0)
    with jax.named_scope("multiply_1a"):
        ring_wait(2, 2)
        multiply(groups[1], 0, 4)
    with jax.named_scope("issue_320"):
        ring_wait(3, 1, 0)
        issue(3, 2, 0)
        issue(2, 3, 0)
    with jax.named_scope("multiply_1b"):
        multiply(groups[1], 5, NZ)
    with jax.named_scope("issue_321"):
        ring_wait(3, 1, 1)
        issue(3, 2, 1)
    with jax.named_scope("multiply_2"):
        multiply(groups[2], 0, 3)
        multiply(groups[2], 6, NZ)
    with jax.named_scope("issue_33"):
        ring_wait(3, 2, 0)
        issue(3, 3, 0)
    with jax.named_scope("wait_23"):
        ring_wait(2, 3, 0)
    with jax.named_scope("spread_1"):
        multiply(groups[1], 4, 5)
        spread_partial(1)
    with jax.named_scope("wait_32"):
        ring_wait(3, 2, 1)
        multiply(groups[2], 3, 4)
        multiply(groups[2], 5, 6)
    with jax.named_scope("total_0"):
        total_and_spread(0)
    with jax.named_scope("last_wait"):
        ring_wait(3, 3, 0)
    with jax.named_scope("spread_2"):
        multiply(groups[2], 4, 5)
        spread_partial(2)
    with jax.named_scope("total_1"):
        total_and_spread(1)
    with jax.named_scope("total_2"):
        total_and_spread(2)

    side = width // NY
    low = side // 2
    tile = 8
    s = y * NX + x
    partner = (x * 2 + 1 - core, c)
    rounds = (
        (6, piece_early, zland_early, packed_early),
        (4, piece_late, zland_late, packed_late),
    )

    def gram_part(turn):
        blocks, part_of, _, _ = rounds[turn]
        count = blocks // 2
        first = s * count // (low // tile)
        for n in range(2):
            b = (first + n) % blocks
            i, j = (b % 3, (b % 3 + b // 3) % 3) if turn == 0 else (b, 3)
            lh, ll = split(proj[:, lanes(i, side)].T)
            rh, rl = split(proj[:, lanes(j, side)])
            block[pl.ds(n * side, side), :] = product(lh, ll, rh, rl)
        for n in range(count):
            at = s * count + n
            row = (at // (low // tile) - first) * side + core * low + at % (low // tile) * tile
            part_of[pl.ds(n * tile, tile), :] = block[pl.ds(pl.multiple_of(row, tile), tile), :]

    def z_all(turn):
        _, part_of, landing, _ = rounds[turn]
        view = landing.at[pl.ds(0, (NZ - 1) * part_of.shape[0]), :]
        return pltpu.make_async_remote_copy(
            src_ref=view, dst_ref=view, send_sem=z_send.at[turn], recv_sem=z_recv.at[turn],
            device_id=z_peer(1), device_id_type=MESH,
        )

    def spread_z(turn):
        _, part_of, landing, _ = rounds[turn]
        own = lanes(z, part_of.shape[0])
        for k in Z_STEPS:
            pltpu.make_async_remote_copy(
                src_ref=part_of, dst_ref=landing.at[own, :],
                send_sem=z_send.at[turn], recv_sem=z_recv.at[turn],
                device_id=z_peer(k), device_id_type=MESH,
            ).start()
        landing[own, :] = part_of[...]

    def packed_rows(turn, of_core, of_y, of_x, chips):
        size = rounds[turn][1].shape[0]
        return pl.ds(pl.multiple_of(((of_core * NY + of_y) * NX + of_x) * size, size), chips * size)

    def spread_gram(turn):
        _, part_of, landing, packed = rounds[turn]
        size = part_of.shape[0]
        z_all(turn).wait_recv()
        total = landing[pl.ds(0, size), :]
        for k in range(1, NZ):
            total = total + landing[pl.ds(k * size, size), :]
        own = packed_rows(turn, core, y, x, 1)
        packed[own, :] = total
        for k in range(PLANE - 1):
            r2, _, c2 = plane_peer(k)
            if turn == 1 or PEERS[k][2] == 0:
                at = PEERS[k][1] if turn == 0 else 0
                pltpu.make_async_remote_copy(
                    src_ref=packed.at[own, :], dst_ref=packed.at[own, :],
                    send_sem=g_send.at[turn], recv_sem=g_recv.at[turn, at],
                    device_id=(r2, c2), device_id_type=MESH,
                ).start()

    def crossing(of_core, ky):
        at = packed_rows(0, of_core, (y - ky + NY) % NY, 0, NX)
        return pltpu.make_async_remote_copy(
            src_ref=packed_early.at[at, :], dst_ref=packed_early.at[at, :],
            send_sem=d_send.at[ky], recv_sem=d_recv.at[ky],
            device_id=partner, device_id_type=MESH,
        )

    def gram_pieces(turn, pieces, at):
        _, part_of, _, packed = rounds[turn]
        view = packed.at[pl.ds(0, pieces * part_of.shape[0]), :]
        return pltpu.make_async_remote_copy(
            src_ref=view, dst_ref=view, send_sem=g_send.at[turn], recv_sem=g_recv.at[turn, at],
            device_id=partner, device_id_type=MESH,
        )

    with jax.named_scope("proj_wait"):
        for group in range(2):
            all_of(proj, group, a_send, a_recv).wait_recv()
    gram_part(0)
    spread_z(0)
    with jax.named_scope("proj_wait_late"):
        all_of(proj, 2, a_send, a_recv).wait_recv()
    gram_part(1)
    spread_z(1)
    with jax.named_scope("z_wait"):
        spread_gram(0)
    with jax.named_scope("z_wait_late"):
        spread_gram(1)
    with jax.named_scope("cross"):
        for ky in (0, 1, 3, 2):
            gram_pieces(0, NX - 1 if ky == 0 else NX, ky).wait_recv()
            crossing(core, ky).start()
    own_cols[...] = proj[lanes(y, cols), :]
    with jax.named_scope("partner_wait"):
        for ky in range(NY):
            crossing(1 - core, ky).wait_recv()
    with jax.named_scope("late_wait"):
        gram_pieces(1, PLANE - 1, 0).wait_recv()

    with jax.named_scope("send_waits"):
        for copy in copies:
            copy.wait_send()
        for k in range(1, NY):
            y_copy(k).wait_send()
        for group in range(3):
            all_of(land, group, p_send, p_recv).wait_send()
            all_of(proj, group, a_send, a_recv).wait_send()
        for turn in range(2):
            z_all(turn).wait_send()
        gram_pieces(0, NX * NY - 1, 0).wait_send()
        gram_pieces(1, PLANE - 1, 0).wait_send()
        for ky in range(NY):
            crossing(core, ky).wait_send()


def polar_kernel(packed_early, packed_late, own_cols, root, right, t, u_hi, u_lo, b_hi, b_lo, v):
    r, c = lax.axis_index("row"), lax.axis_index("col")
    width = t.shape[0]
    cols = own_cols.shape[0]
    wide_len, col_len = root.shape[1], root.shape[0]
    side = width // NY
    low = side // 2
    squares = jnp.zeros((low, side), F32)
    early = [(i, (i + o) % 3) for o in range(2) for i in range(3)]
    for packed, blocks in ((packed_early, early), (packed_late, [(i, 3) for i in range(4)])):
        for b, (i, j) in enumerate(blocks):
            for h in range(2):
                part_of = packed[pl.ds((h * len(blocks) + b) * low, low), :]
                squares = squares + (1.0 if i == j else 2.0) * (part_of * part_of)
                t[pl.ds(i * side + h * low, low), pl.ds(j * side, side)] = part_of
            if i != j:
                t[pl.ds(j * side, side), pl.ds(i * side, side)] = t[
                    pl.ds(i * side, side), pl.ds(j * side, side)
                ].T
    scale = jnp.sqrt(jnp.full((1, 1), jnp.sum(squares), F32) + 1e-06)
    root_scale = jnp.sqrt(scale)
    t[...] = t[...] * (1.0 / scale)

    size = width // 2
    a, b, full = pl.ds(0, size), pl.ds(size, size), pl.ds(0, width)
    tail = pl.ds(width, cols + col_len)
    b_tail = pl.ds(size, size + cols + col_len)
    v[pl.ds(0, cols), :] = own_cols[...]
    v[pl.ds(cols, col_len), :] = t[lanes(c, col_len), :]

    def put(slot, rows, at, value):
        hi, lo = split(value)
        u_hi[slot, rows, at] = hi
        u_lo[slot, rows, at] = lo

    def put_b(rows, at, value):
        hi, lo = split(value)
        b_hi[rows, at] = hi
        b_lo[rows, at] = lo

    def cut(value):
        return value[:size], value[size:]

    put(0, full, full, t[...])
    put(0, tail, full, v[...])
    for step in range(ITERS - 1):
        now, new = step % 2, (step + 1) % 2

        def by_t(rows, at):
            return product(
                u_hi[now, rows, :], u_lo[now, rows, :], u_hi[now, full, at], u_lo[now, full, at]
            )

        def by_b(rows, at):
            return product(u_hi[now, rows, :], u_lo[now, rows, :], b_hi[full, at], b_lo[full, at])

        if step == ITERS - 2:
            def times_t(value):
                hi, lo = split(value)
                both = jnp.concatenate([hi, lo], axis=0)
                dot = functools.partial(jnp.dot, preferred_element_type=F32)
                wide = dot(both, u_hi[now, full, :])
                rows = value.shape[0]
                return (wide[:rows] + wide[rows:]) + dot(hi, u_lo[now, full, :])

            def times_s(value):
                return 1.5 * value - 0.5 * times_t(value)

            value = times_s(v[...])
            v[...] = 1.5 * value - 0.5 * times_s(times_s(times_t(value)))
            break
        value = by_t(a, a)
        put_b(a, a, value)
        t[a, a] = 2.25 * t[a, a] - 1.5 * value
        value, left = cut(by_t(b_tail, a))
        put_b(b, a, value)
        put_b(a, b, value.T)
        t[b, a] = 2.25 * t[b, a] - 1.5 * value
        value, right_half = cut(by_t(b_tail, b))
        put_b(b, b, value)
        t[b, b] = 2.25 * t[b, b] - 1.5 * value
        first, second = cut(by_b(full, a))
        value = t[a, a] + 0.25 * first
        t[a, a] = value
        put(new, a, a, value)
        value = t[b, a] + 0.25 * second
        t[b, a] = value
        put(new, b, a, value)
        put(new, a, b, value.T)
        last = by_b(b, b)
        for at, moved in ((a, left), (b, right_half)):
            value = 1.5 * v[:, at] - 0.5 * moved
            v[:, at] = value
            put(new, tail, at, value)
        value = t[b, b] + 0.25 * last
        t[b, b] = value
        put(new, b, b, value)
    right[...] = v[pl.ds(0, cols), :] * (1.0 / root_scale)
    ours = v[pl.ds(cols, col_len), :] * root_scale
    turn = (width - r * wide_len) % width
    root[...] = pltpu.roll(ours, turn, 1)[:, :wide_len]


def local(matrix, basis):
    cols, depth = matrix.shape
    rows, width = basis.shape
    part = depth // NY
    side = width // NY
    early, late = 6 * side // (2 * NX * NY), 4 * side // (2 * NX * NY)
    row_len, col_len = width // NR, width // (NY * NZ)
    dma = pltpu.SemaphoreType.DMA
    vmem = pl.BlockSpec(memory_space=pltpu.VMEM)
    hbm = pl.BlockSpec(memory_space=pltpu.HBM)
    packed_early, packed_late, own_cols = pl.pallas_call(
        gather_kernel,
        name="gather",
        out_shape=(
            jax.ShapeDtypeStruct((PLANE * early, side), F32),
            jax.ShapeDtypeStruct((PLANE * late, side), F32),
            jax.ShapeDtypeStruct((cols, width), F32),
        ),
        in_specs=[hbm, hbm],
        out_specs=(vmem, vmem, vmem),
        scratch_shapes=[
            pltpu.VMEM((cols, depth), F32),
            pltpu.VMEM((NY * cols, part), F32),
            pltpu.VMEM((NY * cols, part), BF16),
            pltpu.VMEM((NY * cols, part), BF16),
            pltpu.VMEM((NZ * rows, width), F32),
            pltpu.VMEM((NY * cols, width), F32),
            pltpu.VMEM(((PLANE - 1) * cols // NR, width), F32),
            pltpu.VMEM((NY * cols, width), F32),
            pltpu.VMEM((2 * side, side), F32),
            pltpu.VMEM((early, side), F32),
            pltpu.VMEM((late, side), F32),
            pltpu.VMEM((NZ * early, side), F32),
            pltpu.VMEM((NZ * late, side), F32),
            dma((NY - 1,)), dma((NY - 1,)),
            dma((4, 6)), dma((4, 6)), dma((4, 6)), dma((4, 6)), dma((2,)),
            dma((3,)), dma((3,)), dma((3,)), dma((3,)),
            dma((2,)), dma((2,)), dma((2,)), dma((2, NY)), dma((NY,)), dma((NY,)),
            pltpu.SemaphoreType.REGULAR,
        ],
        compiler_params=pltpu.CompilerParams(
            collective_id=0, has_side_effects=True, vmem_limit_bytes=48 * 2**20
        ),
    )(*(pltpu.with_memory_space_constraint(a, pltpu.HBM) for a in (matrix, basis)))
    root, right = pl.pallas_call(
        polar_kernel,
        name="polar",
        out_shape=(
            jax.ShapeDtypeStruct((col_len, row_len), F32),
            jax.ShapeDtypeStruct((cols, width), F32),
        ),
        in_specs=[vmem, vmem, vmem],
        out_specs=(vmem, vmem),
        scratch_shapes=[
            pltpu.VMEM((width, width), F32),
            pltpu.VMEM((2, width + cols + col_len, width), BF16),
            pltpu.VMEM((2, width + cols + col_len, width), BF16),
            pltpu.VMEM((width, width), BF16),
            pltpu.VMEM((width, width), BF16),
            pltpu.VMEM((cols + col_len, width), F32),
        ],
        compiler_params=pltpu.CompilerParams(vmem_limit_bytes=24 * 2**20),
    )(packed_early, packed_late, own_cols)
    return root.T, right


def solution(mesh):
    return jax.shard_map(
        local,
        mesh=mesh,
        in_specs=(P("col", "row"), P(("row", "col"), None)),
        out_specs=(P("row", "col"), P("col", None)),
        check_vma=False,
    )
```

```python
import functools

import jax
import jax.numpy as jnp
from jax import lax
from jax.experimental import pallas as pl
from jax.experimental.pallas import tpu as pltpu
from jax.sharding import PartitionSpec as P

MESH = pl.DeviceIdType.MESH
ITERS = 8
F32 = jnp.float32
BF16 = jnp.bfloat16
NX, NY, NZ = 4, 4, 8
NR, PLANE = 2 * NX, 2 * NX * NY


def split(a):
    hi = a.astype(BF16)
    return hi, (a - hi.astype(F32)).astype(BF16)


def product(ah, al, bh, bl, dims=(((1,), (0,)), ((), ()))):
    dot = functools.partial(
        lax.dot_general, dimension_numbers=dims, preferred_element_type=F32
    )
    return dot(ah, bh) + (dot(ah, bl) + dot(al, bh))


PEERS = sorted(
    [(dx, dy, dc) for dx in range(NX) for dy in range(NY) for dc in range(2)][1:],
    key=lambda p: -(min(p[0], NX - p[0]) * 2 + min(p[1], NY - p[1]) * 2 + p[2]),
)
Z_STEPS = sorted(range(1, NZ), key=lambda d: -min(d, NZ - d))


def lanes(i, size):
    return pl.ds(pl.multiple_of(i * size, size), size)


def gather_kernel(
    mat_hbm, bas_hbm, packed_early, packed_late, own_cols,
    mat, m_in, m_hi, m_lo, q, acc, land, proj, block,
    piece_early, piece_late, zland_early, zland_late,
    y_send, y_recv, f_send, f_recv, b_send, b_recv, local_sem,
    p_send, p_recv, a_send, a_recv, z_send, z_recv, g_send, g_recv, d_send, d_recv, plane_sem,
):
    r, c = lax.axis_index("row"), lax.axis_index("col")
    y, z = c // NZ, c % NZ
    x, core = r // 2, r % 2
    cols = mat.shape[0]
    part = mat.shape[1] // NY
    rows, width = bas_hbm.shape
    half = rows // 2
    wide = width // 4
    piece = cols // NR

    near_x = [(x + d) % NX for d in range(NX)]
    near_y = [(y + d) % NY for d in range(NY)]
    near_row = [[n * 2 + (core + d) % 2 for d in range(2)] for n in near_x]
    near_col = [n * NZ + z for n in near_y]

    def plane_peer(k):
        dx, dy, dc = PEERS[k]
        return near_row[dx][dc], near_y[dy], near_col[dy]

    def z_peer(k):
        return (r, y * NZ + (z + k) % NZ)

    own_basis = pltpu.make_async_copy(bas_hbm, q.at[lanes(z, rows), :], local_sem.at[0])
    own_basis.start()
    own_matrix = pltpu.make_async_copy(mat_hbm, mat, local_sem.at[1])
    own_matrix.start()

    barrier = pltpu.get_barrier_semaphore()

    near = [z_peer(1), z_peer(NZ - 1)] + [(r, near_col[d]) for d in range(1, NY)]
    for k in range(PLANE - 1):
        if PEERS[k][1] == 0:
            near.append((plane_peer(k)[0], c))
    for peer in near:
        pl.semaphore_signal(barrier, inc=1, device_id=peer, device_id_type=MESH)
    with jax.named_scope("barrier"):
        pl.semaphore_wait(barrier, len(near))
    for d in range(1, NY):
        pl.semaphore_signal(plane_sem, inc=1, device_id=(r, near_col[d]), device_id_type=MESH)

    def ring_item(m, d, part, ahead, behind):
        owner = (z - (behind if ahead else -behind) + NZ) % NZ
        span = pl.ds(pl.multiple_of(owner * rows, rows), rows)
        if part is not None:
            start = owner * rows + (0 if ahead == (part == 0) else half)
            span = pl.ds(pl.multiple_of(start, half), half)
        view = q.at[span, pl.ds(m * wide, wide)]
        send, recv = (f_send, f_recv) if ahead else (b_send, b_recv)
        at = d + 3 * (part or 0)
        return pltpu.make_async_remote_copy(
            src_ref=view, dst_ref=view, send_sem=send.at[m, at], recv_sem=recv.at[m, at],
            device_id=(r, y * NZ + (z + (1 if ahead else -1) + NZ) % NZ), device_id_type=MESH,
        )

    def ring_wait(m, d, part=None):
        for ahead in (True, False):
            ring_item(m, d, part, ahead, d + 1).wait_recv()

    def y_copy(k):
        y2 = (y + k) % NY
        return pltpu.make_async_remote_copy(
            src_ref=mat.at[:, lanes(y2, part)], dst_ref=m_in.at[lanes(y, cols), :],
            send_sem=y_send.at[k - 1], recv_sem=y_recv.at[k - 1],
            device_id=(r, y2 * NZ + z), device_id_type=MESH,
        )

    def y_wait(k):
        src = (y - k + NY) % NY
        pltpu.make_async_remote_copy(
            src_ref=mat.at[:, lanes(src, part)], dst_ref=m_in.at[lanes(src, cols), :],
            send_sem=y_send.at[k - 1], recv_sem=y_recv.at[k - 1],
            device_id=(r, src * NZ + z), device_id_type=MESH,
        ).wait_recv()

    copies = []

    def issue(m, d, part=None):
        for ahead in (True, False):
            copy = ring_item(m, d, part, ahead, d)
            copy.start()
            copies.append(copy)

    def split_rows(src):
        def one(i, _):
            at = pl.ds(pl.multiple_of(i * 16, 16), 16)
            hi, lo = split(m_in[at, :])
            m_hi[at, :] = hi
            m_lo[at, :] = lo
            return 0

        lax.fori_loop(src * (cols // 16), (src + 1) * (cols // 16), one, 0)

    def own_split(i, _):
        hi, lo = split(mat[pl.ds(pl.multiple_of(i * 16, 16), 16), lanes(y, part)])
        at = pl.ds(pl.multiple_of(y * cols + i * 16, 16), 16)
        m_hi[at, :] = hi
        m_lo[at, :] = lo
        return 0

    groups = [pl.ds(0, 2 * wide), pl.ds(2 * wide, wide), pl.ds(3 * wide, wide)]

    def multiply(here, first, last):

        def one(o, _):
            owner = (z + o) % NZ
            qh, ql = split(q[lanes(owner, rows), here])
            at = lanes(owner, rows)
            acc[:, here] += product(m_hi[:, at], m_lo[:, at], qh, ql)
            return 0

        lax.fori_loop(first, last, one, 0)

    def spread_partial(group, steps=range(NY)):
        here = groups[group]
        for k in range(PLANE - 1):
            if PEERS[k][1] not in steps:
                continue
            r2, y2, c2 = plane_peer(k)
            src = pl.ds(pl.multiple_of(y2 * cols + r2 * piece, piece), piece)
            pltpu.make_async_remote_copy(
                src_ref=acc.at[src, here], dst_ref=land.at[pl.ds(k * piece, piece), here],
                send_sem=p_send.at[group], recv_sem=p_recv.at[group],
                device_id=(r2, c2), device_id_type=MESH,
            ).start()

    mine = pl.ds(pl.multiple_of(y * cols + r * piece, piece), piece)

    def all_of(ref, group, send, recv):
        view = ref.at[pl.ds(0, (PLANE - 1) * piece), groups[group]]
        return pltpu.make_async_remote_copy(
            src_ref=view, dst_ref=view, send_sem=send.at[group], recv_sem=recv.at[group],
            device_id=z_peer(1), device_id_type=MESH,
        )

    def total_and_spread(group):
        here = groups[group]
        all_of(land, group, p_send, p_recv).wait_recv()
        total = acc[mine, here]
        for k in range(PLANE - 1):
            total = total + land[pl.ds(k * piece, piece), here]
        proj[mine, here] = total

        for k in range(PLANE - 1):
            r2, _, c2 = plane_peer(k)
            pltpu.make_async_remote_copy(
                src_ref=proj.at[mine, here], dst_ref=proj.at[mine, here],
                send_sem=a_send.at[group], recv_sem=a_recv.at[group],
                device_id=(r2, c2), device_id_type=MESH,
            ).start()

    own_basis.wait()
    issue(0, 0)
    own_matrix.wait()
    for k in range(1, NY):
        y_copy(k).start()
    issue(1, 0)
    acc[...] = jnp.zeros_like(acc)
    lax.fori_loop(0, cols // 16, own_split, 0)
    for m, d in ((0, 1), (1, 1), (0, 2), (1, 2)):
        with jax.named_scope(f"issue_{m}{d}"):
            ring_wait(m, d - 1)
            issue(m, d)
    issue(2, 0)
    issue(3, 0)
    with jax.named_scope("issue_21"):
        for m in (0, 1):
            ring_wait(m, 2)
        ring_wait(2, 0)
        issue(2, 1)
    issue(0, 3, 0)
    issue(1, 3, 0)
    with jax.named_scope("issue_31"):
        ring_wait(3, 0)
    with jax.named_scope("issue_22"):
        ring_wait(2, 1)
        issue(2, 2)
    for which in (0, 1):
        issue(3, 1, which)
    with jax.named_scope("y_wait"):
        for k in range(1, NY):
            y_wait(k)
            split_rows((y - k + NY) % NY)
    with jax.named_scope("multiply_0"):
        multiply(groups[0], 0, 4)
        multiply(groups[0], 5, NZ)
    with jax.named_scope("wait_03"):
        for m in (0, 1):
            ring_wait(m, 3, 0)
        multiply(groups[0], 4, 5)
    with jax.named_scope("spread_0"):
        pl.semaphore_wait(plane_sem, NY - 1)
        spread_partial(0)
    with jax.named_scope("multiply_1a"):
        ring_wait(2, 2)
        multiply(groups[1], 0, 4)
    with jax.named_scope("issue_320"):
        ring_wait(3, 1, 0)
        issue(3, 2, 0)
        issue(2, 3, 0)
    with jax.named_scope("multiply_1b"):
        multiply(groups[1], 5, NZ)
    with jax.named_scope("issue_321"):
        ring_wait(3, 1, 1)
        issue(3, 2, 1)
    with jax.named_scope("multiply_2"):
        multiply(groups[2], 0, 3)
        multiply(groups[2], 6, NZ)
    with jax.named_scope("issue_33"):
        ring_wait(3, 2, 0)
        issue(3, 3, 0)
    with jax.named_scope("wait_23"):
        ring_wait(2, 3, 0)
    with jax.named_scope("spread_1"):
        multiply(groups[1], 4, 5)
        spread_partial(1)
    with jax.named_scope("wait_32"):
        ring_wait(3, 2, 1)
        multiply(groups[2], 3, 4)
        multiply(groups[2], 5, 6)
    with jax.named_scope("total_0"):
        total_and_spread(0)
    with jax.named_scope("last_wait"):
        ring_wait(3, 3, 0)
    with jax.named_scope("spread_2"):
        at = lanes((z + 4) % NZ, rows)
        qh, ql = split(q[at, groups[2]])
        for steps in ((2,), (1, 3, 0)):
            for d in steps:
                own = lanes(near_y[d], cols)
                acc[own, groups[2]] += product(m_hi[own, at], m_lo[own, at], qh, ql)
            spread_partial(2, steps)
    with jax.named_scope("total_1"):
        total_and_spread(1)
    with jax.named_scope("total_2"):
        total_and_spread(2)

    side = width // NY
    low = side // 2
    tile = 8
    s = y * NX + x
    partner = (x * 2 + 1 - core, c)
    rounds = (
        (6, piece_early, zland_early, packed_early),
        (4, piece_late, zland_late, packed_late),
    )

    def gram_part(turn):
        blocks, part_of, _, _ = rounds[turn]
        count = blocks // 2
        first = s * count // (low // tile)
        for n in range(2):
            b = (first + n) % blocks
            i, j = (b % 3, (b % 3 + b // 3) % 3) if turn == 0 else (b, 3)
            lh, ll = split(proj[:, lanes(i, side)].T)
            rh, rl = split(proj[:, lanes(j, side)])
            block[pl.ds(n * side, side), :] = product(lh, ll, rh, rl)
        for n in range(count):
            at = s * count + n
            row = (at // (low // tile) - first) * side + core * low + at % (low // tile) * tile
            part_of[pl.ds(n * tile, tile), :] = block[pl.ds(pl.multiple_of(row, tile), tile), :]

    def z_all(turn):
        _, part_of, landing, _ = rounds[turn]
        view = landing.at[pl.ds(0, (NZ - 1) * part_of.shape[0]), :]
        return pltpu.make_async_remote_copy(
            src_ref=view, dst_ref=view, send_sem=z_send.at[turn], recv_sem=z_recv.at[turn],
            device_id=z_peer(1), device_id_type=MESH,
        )

    def spread_z(turn):
        _, part_of, landing, _ = rounds[turn]
        own = lanes(z, part_of.shape[0])
        for k in Z_STEPS:
            pltpu.make_async_remote_copy(
                src_ref=part_of, dst_ref=landing.at[own, :],
                send_sem=z_send.at[turn], recv_sem=z_recv.at[turn],
                device_id=z_peer(k), device_id_type=MESH,
            ).start()
        landing[own, :] = part_of[...]

    def packed_rows(turn, of_core, of_y, of_x, chips):
        size = rounds[turn][1].shape[0]
        return pl.ds(pl.multiple_of(((of_core * NY + of_y) * NX + of_x) * size, size), chips * size)

    def spread_gram(turn):
        _, part_of, landing, packed = rounds[turn]
        size = part_of.shape[0]
        z_all(turn).wait_recv()
        total = landing[pl.ds(0, size), :]
        for k in range(1, NZ):
            total = total + landing[pl.ds(k * size, size), :]
        own = packed_rows(turn, core, y, x, 1)
        packed[own, :] = total
        for k in range(PLANE - 1):
            r2, _, c2 = plane_peer(k)
            if turn == 1 or PEERS[k][2] == 0:
                at = PEERS[k][1] if turn == 0 else 0
                pltpu.make_async_remote_copy(
                    src_ref=packed.at[own, :], dst_ref=packed.at[own, :],
                    send_sem=g_send.at[turn], recv_sem=g_recv.at[turn, at],
                    device_id=(r2, c2), device_id_type=MESH,
                ).start()

    def crossing(of_core, ky):
        at = packed_rows(0, of_core, (y - ky + NY) % NY, 0, NX)
        return pltpu.make_async_remote_copy(
            src_ref=packed_early.at[at, :], dst_ref=packed_early.at[at, :],
            send_sem=d_send.at[ky], recv_sem=d_recv.at[ky],
            device_id=partner, device_id_type=MESH,
        )

    def gram_pieces(turn, pieces, at):
        _, part_of, _, packed = rounds[turn]
        view = packed.at[pl.ds(0, pieces * part_of.shape[0]), :]
        return pltpu.make_async_remote_copy(
            src_ref=view, dst_ref=view, send_sem=g_send.at[turn], recv_sem=g_recv.at[turn, at],
            device_id=partner, device_id_type=MESH,
        )

    with jax.named_scope("proj_wait"):
        for group in range(2):
            all_of(proj, group, a_send, a_recv).wait_recv()
    gram_part(0)
    spread_z(0)
    with jax.named_scope("proj_wait_late"):
        all_of(proj, 2, a_send, a_recv).wait_recv()
    gram_part(1)
    spread_z(1)
    with jax.named_scope("z_wait"):
        spread_gram(0)
    with jax.named_scope("z_wait_late"):
        spread_gram(1)
    with jax.named_scope("cross"):
        for ky in (0, 1, 3, 2):
            gram_pieces(0, NX - 1 if ky == 0 else NX, ky).wait_recv()
            crossing(core, ky).start()
    own_cols[...] = proj[lanes(y, cols), :]
    with jax.named_scope("partner_wait"):
        for ky in range(NY):
            crossing(1 - core, ky).wait_recv()
    with jax.named_scope("late_wait"):
        gram_pieces(1, PLANE - 1, 0).wait_recv()

    with jax.named_scope("send_waits"):
        for copy in copies:
            copy.wait_send()
        for k in range(1, NY):
            y_copy(k).wait_send()
        for group in range(3):
            all_of(land, group, p_send, p_recv).wait_send()
            all_of(proj, group, a_send, a_recv).wait_send()
        for turn in range(2):
            z_all(turn).wait_send()
        gram_pieces(0, NX * NY - 1, 0).wait_send()
        gram_pieces(1, PLANE - 1, 0).wait_send()
        for ky in range(NY):
            crossing(core, ky).wait_send()


def polar_kernel(packed_early, packed_late, own_cols, root, right, t, u_hi, u_lo, b_hi, b_lo, v):
    r, c = lax.axis_index("row"), lax.axis_index("col")
    width = t.shape[0]
    cols = own_cols.shape[0]
    wide_len, col_len = root.shape[1], root.shape[0]
    side = width // NY
    low = side // 2
    squares = jnp.zeros((low, side), F32)
    early = [(i, (i + o) % 3) for o in range(2) for i in range(3)]
    for packed, blocks in ((packed_early, early), (packed_late, [(i, 3) for i in range(4)])):
        for b, (i, j) in enumerate(blocks):
            for h in range(2):
                part_of = packed[pl.ds((h * len(blocks) + b) * low, low), :]
                squares = squares + (1.0 if i == j else 2.0) * (part_of * part_of)
                t[pl.ds(i * side + h * low, low), pl.ds(j * side, side)] = part_of
            if i != j:
                t[pl.ds(j * side, side), pl.ds(i * side, side)] = t[
                    pl.ds(i * side, side), pl.ds(j * side, side)
                ].T
    scale = jnp.sqrt(jnp.full((1, 1), jnp.sum(squares), F32) + 1e-06)
    root_scale = jnp.sqrt(scale)
    t[...] = t[...] * (1.0 / scale)

    size = width // 2
    a, b, full = pl.ds(0, size), pl.ds(size, size), pl.ds(0, width)
    tail = pl.ds(width, cols + col_len)
    b_tail = pl.ds(size, size + cols + col_len)
    v[pl.ds(0, cols), :] = own_cols[...]
    v[pl.ds(cols, col_len), :] = t[lanes(c, col_len), :]

    def put(slot, rows, at, value):
        hi, lo = split(value)
        u_hi[slot, rows, at] = hi
        u_lo[slot, rows, at] = lo

    def put_b(rows, at, value):
        hi, lo = split(value)
        b_hi[rows, at] = hi
        b_lo[rows, at] = lo

    def cut(value):
        return value[:size], value[size:]

    put(0, full, full, t[...])
    put(0, tail, full, v[...])
    for step in range(ITERS - 1):
        now, new = step % 2, (step + 1) % 2

        def by_t(rows, at):
            return product(
                u_hi[now, rows, :], u_lo[now, rows, :], u_hi[now, full, at], u_lo[now, full, at]
            )

        def by_b(rows, at):
            return product(u_hi[now, rows, :], u_lo[now, rows, :], b_hi[full, at], b_lo[full, at])

        if step == ITERS - 2:
            def times_t(value):
                hi, lo = split(value)
                both = jnp.concatenate([hi, lo], axis=0)
                dot = functools.partial(jnp.dot, preferred_element_type=F32)
                wide = dot(both, u_hi[now, full, :])
                rows = value.shape[0]
                return (wide[:rows] + wide[rows:]) + dot(hi, u_lo[now, full, :])

            def times_s(value):
                return 1.5 * value - 0.5 * times_t(value)

            value = times_s(v[...])
            v[...] = 1.5 * value - 0.5 * times_s(times_s(times_t(value)))
            break
        value = by_t(a, a)
        put_b(a, a, value)
        t[a, a] = 2.25 * t[a, a] - 1.5 * value
        value, left = cut(by_t(b_tail, a))
        put_b(b, a, value)
        put_b(a, b, value.T)
        t[b, a] = 2.25 * t[b, a] - 1.5 * value
        value, right_half = cut(by_t(b_tail, b))
        put_b(b, b, value)
        t[b, b] = 2.25 * t[b, b] - 1.5 * value
        first, second = cut(by_b(full, a))
        value = t[a, a] + 0.25 * first
        t[a, a] = value
        put(new, a, a, value)
        value = t[b, a] + 0.25 * second
        t[b, a] = value
        put(new, b, a, value)
        put(new, a, b, value.T)
        last = by_b(b, b)
        for at, moved in ((a, left), (b, right_half)):
            value = 1.5 * v[:, at] - 0.5 * moved
            v[:, at] = value
            put(new, tail, at, value)
        value = t[b, b] + 0.25 * last
        t[b, b] = value
        put(new, b, b, value)
    right[...] = v[pl.ds(0, cols), :] * (1.0 / root_scale)
    ours = v[pl.ds(cols, col_len), :] * root_scale
    turn = (width - r * wide_len) % width
    root[...] = pltpu.roll(ours, turn, 1)[:, :wide_len]


def local(matrix, basis):
    cols, depth = matrix.shape
    rows, width = basis.shape
    part = depth // NY
    side = width // NY
    early, late = 6 * side // (2 * NX * NY), 4 * side // (2 * NX * NY)
    row_len, col_len = width // NR, width // (NY * NZ)
    dma = pltpu.SemaphoreType.DMA
    vmem = pl.BlockSpec(memory_space=pltpu.VMEM)
    hbm = pl.BlockSpec(memory_space=pltpu.HBM)
    packed_early, packed_late, own_cols = pl.pallas_call(
        gather_kernel,
        name="gather",
        out_shape=(
            jax.ShapeDtypeStruct((PLANE * early, side), F32),
            jax.ShapeDtypeStruct((PLANE * late, side), F32),
            jax.ShapeDtypeStruct((cols, width), F32),
        ),
        in_specs=[hbm, hbm],
        out_specs=(vmem, vmem, vmem),
        scratch_shapes=[
            pltpu.VMEM((cols, depth), F32),
            pltpu.VMEM((NY * cols, part), F32),
            pltpu.VMEM((NY * cols, part), BF16),
            pltpu.VMEM((NY * cols, part), BF16),
            pltpu.VMEM((NZ * rows, width), F32),
            pltpu.VMEM((NY * cols, width), F32),
            pltpu.VMEM(((PLANE - 1) * cols // NR, width), F32),
            pltpu.VMEM((NY * cols, width), F32),
            pltpu.VMEM((2 * side, side), F32),
            pltpu.VMEM((early, side), F32),
            pltpu.VMEM((late, side), F32),
            pltpu.VMEM((NZ * early, side), F32),
            pltpu.VMEM((NZ * late, side), F32),
            dma((NY - 1,)), dma((NY - 1,)),
            dma((4, 6)), dma((4, 6)), dma((4, 6)), dma((4, 6)), dma((2,)),
            dma((3,)), dma((3,)), dma((3,)), dma((3,)),
            dma((2,)), dma((2,)), dma((2,)), dma((2, NY)), dma((NY,)), dma((NY,)),
            pltpu.SemaphoreType.REGULAR,
        ],
        compiler_params=pltpu.CompilerParams(
            collective_id=0, has_side_effects=True, vmem_limit_bytes=48 * 2**20
        ),
    )(*(pltpu.with_memory_space_constraint(a, pltpu.HBM) for a in (matrix, basis)))
    root, right = pl.pallas_call(
        polar_kernel,
        name="polar",
        out_shape=(
            jax.ShapeDtypeStruct((col_len, row_len), F32),
            jax.ShapeDtypeStruct((cols, width), F32),
        ),
        in_specs=[vmem, vmem, vmem],
        out_specs=(vmem, vmem),
        scratch_shapes=[
            pltpu.VMEM((width, width), F32),
            pltpu.VMEM((2, width + cols + col_len, width), BF16),
            pltpu.VMEM((2, width + cols + col_len, width), BF16),
            pltpu.VMEM((width, width), BF16),
            pltpu.VMEM((width, width), BF16),
            pltpu.VMEM((cols + col_len, width), F32),
        ],
        compiler_params=pltpu.CompilerParams(vmem_limit_bytes=24 * 2**20),
    )(packed_early, packed_late, own_cols)
    return root.T, right


def solution(mesh):
    return jax.shard_map(
        local,
        mesh=mesh,
        in_specs=(P("col", "row"), P(("row", "col"), None)),
        out_specs=(P("row", "col"), P("col", None)),
        check_vma=False,
    )
```
